32 devices in a mesh: shard: 32 (over z, y, x, core).
Axes of the slice: x: 2, y: 2, z: 4, core: 2. Of those that a mesh axis runs over, the one named last changes fastest.
Arguments:
- data_t: bfloat16 [8192, 8192], P('shard'), may hold values from -0.125 to 0.125
- labels: int32 [8192], replicated, may hold values from -1 to 1, as said below
- sample_weight: float32 [8192], replicated, may hold values from 0.1 to 4
- w_start: float32 [8192], P('shard'), may hold values from -10 to 10
- alpha_start: float32 [8192], P('shard'), may hold values from 0 to 1
- visit_order: int32 [64, 128], P('shard'), may hold values from 0 to 127, each once within a row
Outputs:
- weights_out: float32 [8192], P('shard')
- alpha_final: float32 [8192], P('shard')
- objective: float32 [], replicated
The draws below stay inside these ranges and needn't reach their ends.
Inputs may be any that keep to these rules, and one draw needn't show every extreme that they name: `labels`: each label is -1 or +1. `visit_order`: each row is a permutation of 0 to 127.
All inputs are finite; a program needn't handle non-finite values.
Results may differ from the reference program's by a relative error of at most 0.0047.
Values may be sent and summed in bfloat16 or wider, within the bound.
A program may use at most 64 MiB of HBM per device.

```python
import jax
import jax.numpy as jnp
from jax import lax

FEATURES = 8192
BLOCK = 128
GROUP = 16
SAMPLES = 8192
BLOCKS = 64
N_SHARD = 32


def draw_labels(key, part):
    return (2 * jax.random.randint(key, (SAMPLES,), 0, 2) - 1).astype(jnp.int32)


def draw_sample_weight(key, part):
    position = jnp.arange(SAMPLES, dtype=jnp.float32) / (SAMPLES - 1)
    roughness = jnp.exp(jax.random.uniform(key, (SAMPLES,), jnp.float32, -0.35, 0.35))
    return (0.5 * jnp.power(3.0, position) * roughness).astype(jnp.float32)


def draw_w_start(key, part):
    position = jnp.arange(FEATURES, dtype=jnp.float32) / (FEATURES - 1)
    normal_draw = jnp.clip(jax.random.normal(key, (FEATURES,), jnp.float32), -4.0, 4.0)
    return (0.6 * jnp.power(3.0, position) * normal_draw).astype(jnp.float32)


def with_spikes(array, stream_key, source, target, parts, factor):
    owner, partner = [(jnp.arange(array.shape[axis_at]) // (array.shape[axis_at] // parts)).reshape([-1 if axis == axis_at else 1 for axis in range(array.ndim)]) for axis_at in (source, target)]
    chosen = jax.random.permutation(stream_key, parts)[partner]
    strong = (owner == chosen) | (owner == (partner + parts // 2) % parts)
    return jnp.where(strong, factor * array, array)


def steps_of(stream_key, dims, cuts, smallest, high):
    factor_of, own = 1.0, jax.random.fold_in(stream_key, 6)
    for dim, shards_of in cuts:
        heights = jnp.exp(jax.random.uniform(jax.random.fold_in(own, dim), (shards_of,), jnp.float32, smallest / len(cuts), high / len(cuts)))
        factor_of = factor_of * jnp.repeat(heights, dims[dim] // shards_of).reshape([-1 if axis == dim else 1 for axis in range(len(dims))])
    return factor_of


def noise_with(own_key, shape, spread, limit, cuts, heavy, held_as=jnp.bfloat16):
    array = spread * jax.random.normal(own_key, shape, jnp.float32)
    if cuts:
        array = array * steps_of(own_key, shape, cuts, -0.22, 0.18)
    return jnp.clip(with_spikes(array, jax.random.fold_in(own_key, 3), *heavy), -limit, limit).astype(held_as)


def setup_inputs(seed: int = 0) -> dict:
    key_of = jax.random.split(jax.random.key(seed), 7)
    return {
        "data_t": noise_with(key_of[0], (FEATURES, SAMPLES), FEATURES ** -0.5, 0.125, ((0, 32),), (1, 0, 32, 2.75)),
        "labels": draw_labels(jax.random.fold_in(key_of[6], 71), 0),
        "sample_weight": draw_sample_weight(jax.random.fold_in(key_of[6], 71), 0),
        "w_start": draw_w_start(jax.random.fold_in(key_of[6], 71), 0),
        "alpha_start": jnp.clip(1.0 * jax.random.uniform(key_of[4], (SAMPLES,), jnp.float32) ** steps_of(key_of[4], (SAMPLES,), ((0, 32),), -0.2, 0.2), 0.0, 1.0),
        "visit_order": jax.vmap(lambda own: jax.random.permutation(own, BLOCK))(jax.random.split(key_of[5], BLOCKS)).reshape((BLOCKS, BLOCK)).astype(jnp.int32),
    }


def sweep_rows(gram_block, label_rows, bound_rows, alpha_rows, margin_rows, visit_rows):
    gram_perm = gram_block[visit_rows][:, visit_rows]
    label_perm = label_rows[visit_rows]
    bound_perm = bound_rows[visit_rows]
    alpha_perm = alpha_rows[visit_rows]
    margin_perm = margin_rows[visit_rows]
    diag_perm = jnp.diagonal(gram_perm) + 1e-6

    def update_group(group_index, state_pair):
        alpha_now, margin_now = state_pair
        first_row = jnp.asarray(group_index * GROUP).astype(jnp.int32)
        group_alpha = lax.dynamic_slice_in_dim(alpha_now, first_row, GROUP)
        group_label = lax.dynamic_slice_in_dim(label_perm, first_row, GROUP)
        group_margin = lax.dynamic_slice_in_dim(margin_now, first_row, GROUP)
        group_diag = lax.dynamic_slice_in_dim(diag_perm, first_row, GROUP)
        group_bound = lax.dynamic_slice_in_dim(bound_perm, first_row, GROUP)
        fresh_alpha = jnp.clip(group_alpha + (1.0 - group_label * group_margin) / (2.0 * group_diag), 0.0, group_bound)
        change = fresh_alpha - group_alpha
        columns = lax.dynamic_slice_in_dim(gram_perm, first_row, GROUP, 1)
        margin_now = margin_now + 2.0 * jnp.dot(columns, group_label * change, precision=lax.Precision.HIGHEST)
        alpha_now = lax.dynamic_update_slice_in_dim(alpha_now, fresh_alpha, first_row, 0)
        return alpha_now, margin_now

    alpha_perm, margin_perm = lax.fori_loop(0, alpha_rows.shape[0] // GROUP, update_group, (alpha_perm, margin_perm))
    return jnp.zeros_like(alpha_rows).at[visit_rows].set(alpha_perm)


def reference(data_t, labels, sample_weight, w_start, alpha_start, visit_order):
    features, samples = data_t.shape
    devices = N_SHARD
    row_count = samples // devices
    label_sign = labels.astype(jnp.float32)
    start_margin = jnp.dot(w_start.astype(jnp.bfloat16), data_t, preferred_element_type=jnp.float32)
    weighted = (sample_weight * label_sign * jnp.maximum(0.0, 1.0 - label_sign * start_margin)).astype(jnp.bfloat16)
    ascent = jnp.dot(data_t, weighted, preferred_element_type=jnp.float32)
    column_sq = jnp.einsum("fs,fs->f", data_t, data_t, preferred_element_type=jnp.float32)
    scale_col = column_sq / samples + 1e-6
    stepped = w_start + ascent / (samples * scale_col)
    thresh = 1.0 / (4.0 * features * scale_col)
    primal = stepped - jnp.clip(stepped, -thresh, thresh)
    model_margin = jnp.dot(primal.astype(jnp.bfloat16), data_t, preferred_element_type=jnp.float32)
    objective = jnp.sum(sample_weight * jnp.square(jnp.maximum(0.0, 1.0 - label_sign * model_margin))) / (2.0 * samples) + jnp.sum(jnp.abs(primal)) / (4.0 * features)
    block_count = row_count // BLOCK
    visit_rows = visit_order.reshape(devices, block_count, BLOCK) + (jnp.arange(block_count, dtype=jnp.int32) * BLOCK)[None, :, None]
    visit_rows = visit_rows.reshape(devices, row_count).astype(jnp.int32)

    def gram_one(device_number):
        first = (device_number * row_count).astype(jnp.int32)
        piece = lax.dynamic_slice_in_dim(data_t, first, row_count, 1)
        return lax.dot_general(piece, piece, (((0,), (0,)), ((), ())), preferred_element_type=jnp.float32)

    gram_all = lax.map(gram_one, jnp.arange(devices, dtype=jnp.int32))
    sign_dev = label_sign.reshape(devices, row_count)
    bound_dev = sample_weight.reshape(devices, row_count)
    alpha_zero = bound_dev * alpha_start.reshape(devices, row_count)
    sweep_all = jax.vmap(sweep_rows)
    alpha_one = sweep_all(gram_all, sign_dev, bound_dev, alpha_zero, model_margin.reshape(devices, row_count), visit_rows)
    change_one = (sign_dev * (alpha_one - alpha_zero)).reshape(samples).astype(jnp.bfloat16)
    update_one = jnp.dot(data_t, change_one, preferred_element_type=jnp.float32) * (2.0 / devices)
    second_margin = model_margin + jnp.dot(update_one.astype(jnp.bfloat16), data_t, preferred_element_type=jnp.float32)
    alpha_two = sweep_all(gram_all, sign_dev, bound_dev, alpha_one, second_margin.reshape(devices, row_count), visit_rows)
    change_two = (sign_dev * (alpha_two - alpha_one)).reshape(samples).astype(jnp.bfloat16)
    update_two = jnp.dot(data_t, change_two, preferred_element_type=jnp.float32) * (2.0 / devices)
    weights_out = primal + update_one + update_two
    return weights_out, alpha_two.reshape(samples), objective
```

```python
import functools

import jax
import jax.numpy as jnp
from jax import lax
from jax.experimental import pallas as pl
from jax.experimental.pallas import tpu as pltpu
from jax.sharding import PartitionSpec as P

GROUP = 16
ROWS = 16
MESH = pl.DeviceIdType.MESH
F32 = jnp.float32
BF16 = jnp.bfloat16
HIGH = lax.Precision.HIGHEST


def nn(a, b, precision=None):
    return lax.dot_general(a, b, (((1,), (0,)), ((), ())), preferred_element_type=F32, precision=precision)


def nt(a, b, precision=None):
    return lax.dot_general(a, b, (((1,), (1,)), ((), ())), preferred_element_type=F32, precision=precision)


def spread(row):
    return jnp.broadcast_to(row, (ROWS, row.shape[-1])).astype(BF16)


def kernel(
    devices, data_ref, sign_ref, bound_ref, start_ref, frac_ref, visit_ref,
    weight_ref, alpha_ref, objective_ref,
    part0, part1, part2, got0, got1, got2, own0, own1, own2, all0, all1, all2,
    gram, pair_in, pair_sum, gram_in,
    send_sem, recv_sem, pair_send, pair_recv, gram_send, gram_recv,
):
    me = lax.axis_index("shard")
    feats, samples = data_ref.shape
    rows = sign_ref.shape[1]
    blocks, block = visit_ref.shape
    features = feats * devices
    chips = devices // 2
    chip, core = me // 2, me % 2
    partner = 2 * chip + 1 - core

    def columns(k):
        return pl.ds(pl.multiple_of(k * rows, rows), rows)

    def peers(action):
        def step(i, carry):
            action(lax.rem(me + i, devices))
            return carry

        lax.fori_loop(1, devices, step, 0)

    def total_wait(ref, phase):
        view = ref.at[pl.ds(0, devices - 1)]
        return pltpu.make_async_remote_copy(
            src_ref=view, dst_ref=view, send_sem=send_sem.at[phase], recv_sem=recv_sem.at[phase],
            device_id=(partner,), device_id_type=MESH,
        )

    def scatter_start(part, got, phase):
        def send(peer):
            pltpu.make_async_remote_copy(
                src_ref=part.at[peer], dst_ref=got.at[me], send_sem=send_sem.at[phase],
                recv_sem=recv_sem.at[phase], device_id=(peer,), device_id_type=MESH,
            ).start()

        peers(send)
        got[me] = part[me]

    def gather_start(own, everyone, phase):
        def send(peer):
            pltpu.make_async_remote_copy(
                src_ref=own, dst_ref=everyone.at[me], send_sem=send_sem.at[phase],
                recv_sem=recv_sem.at[phase], device_id=(peer,), device_id_type=MESH,
            ).start()

        peers(send)
        everyone[me] = own[...]

    def margin_parts(row, part):
        lhs = spread(row)

        def step(k, carry):
            part[k, 0:1, :] = nn(lhs, data_ref[:, columns(k)])[0:1, :]
            return carry

        lax.fori_loop(0, devices, step, 0, unroll=4)

    def back(everyone):
        def step(k, total):
            return total + nt(spread(everyone[k][0:1, 0:rows]), data_ref[:, columns(k)])

        return lax.fori_loop(0, devices, step, jnp.zeros((ROWS, feats), F32), unroll=4)[0:1, :]

    barrier = pltpu.get_barrier_semaphore()
    peers(lambda peer: pl.semaphore_signal(barrier, inc=1, device_id=(peer,), device_id_type=MESH))

    w_start = start_ref[...]
    sign, bound = sign_ref[...], bound_ref[...]
    margin_parts(w_start, part0)
    pl.semaphore_wait(barrier, devices - 1)
    scatter_start(part0, got0, 0)

    def gram_of(k):
        tile = data_ref[:, columns(k)]
        offset = 0
        for a in range(blocks):
            width = rows - a * block
            piece = lax.dot_general(
                tile[:, a * block:(a + 1) * block], tile[:, a * block:],
                (((0,), (0,)), ((), ())), preferred_element_type=F32,
            )
            gram[k, :, offset:offset + width] = piece.astype(BF16)
            offset += width
        square = tile.astype(F32)
        square = square * square
        part1[k, 1:2, :] = jnp.sum(square, axis=0, keepdims=True)
        return square

    def pair_copy(c):
        return pltpu.make_async_remote_copy(
            src_ref=gram.at[2 * c + 1 - core], dst_ref=pair_in.at[c], send_sem=pair_send.at[c],
            recv_sem=pair_recv.at[c], device_id=(partner,), device_id_type=MESH,
        )

    def gram_step(i, total):
        c = lax.rem(chip + 1 + i, chips)
        square = gram_of(2 * c + 1 - core)
        pair_copy(c).start()
        return total + square + gram_of(2 * c + core)

    square_total = lax.fori_loop(0, chips, gram_step, jnp.zeros((feats, rows), F32))
    column_sq = nt(jnp.ones((8, rows), F32), square_total, HIGH)[0:1, :]

    total_wait(got0, 0).wait_recv()
    margin0 = jnp.sum(got0[...], axis=0)
    own0[...] = bound * sign * jnp.maximum(0.0, 1.0 - sign * margin0)
    gather_start(own0, all0, 0 + 3)

    def gram_copy(c):
        return pltpu.make_async_remote_copy(
            src_ref=pair_sum.at[c], dst_ref=gram_in.at[chip], send_sem=gram_send.at[0],
            recv_sem=gram_recv.at[0], device_id=(2 * c + core,), device_id_type=MESH,
        )

    def merged(c):
        pair_copy(c).wait_recv()
        return (gram[2 * c + core].astype(F32) + pair_in[c].astype(F32)).astype(BF16)

    def merge_step(i, carry):
        c = lax.rem(chip + 1 + i, chips)
        pair_sum[c] = merged(c)
        gram_copy(c).start()
        return carry

    lax.fori_loop(0, chips - 1, merge_step, 0)
    gram_in[chip] = merged(chip)

    total_wait(all0, 3).wait_recv()
    ascent = back(all0)
    scale = column_sq / samples + 1e-06
    stepped = w_start + ascent / (samples * scale)
    thresh = 1.0 / (4.0 * features * scale)
    primal = stepped - jnp.clip(stepped, -thresh, thresh)
    margin_parts(primal, part1)
    scatter_start(part1, got1, 1)

    orders, places = [], []
    for b in range(blocks):
        order = (lax.broadcasted_iota(jnp.int32, (block, block), 0) == visit_ref[b:b + 1, :]).astype(F32)
        orders.append(order)
        places.append(order.T.astype(BF16))

    alpha_zero = bound * frac_ref[...]

    def permute(vectors):
        stacked = jnp.concatenate(list(vectors) + [jnp.zeros((8 - len(vectors), rows), F32)], axis=0)
        return [nn(stacked[:, b * block:(b + 1) * block], orders[b], HIGH) for b in range(blocks)]

    total_wait(got1, 1).wait_recv()
    received = jnp.sum(got1[...], axis=0)
    margin1, diag = received[0:1, :], received[1:2, :]
    loss = jnp.sum(bound * jnp.square(jnp.maximum(0.0, 1.0 - sign * margin1)), axis=1, keepdims=True)
    penalty = jnp.sum(jnp.abs(primal), axis=1, keepdims=True)
    objective_part = loss / (2.0 * samples) + penalty / (4.0 * features)
    permuted = permute((sign, bound, alpha_zero, diag, margin1))
    sign_p = [x[0:1] for x in permuted]
    bound_p = [x[1:2] for x in permuted]
    zero_p = [x[2:3] for x in permuted]
    inverse_p = [0.5 / (x[3:4] + 1e-06) for x in permuted]
    margin_p = [x[4:5] for x in permuted]

    view = gram_in.at[pl.ds(0, chips - 1)]
    gram_wait = pltpu.make_async_remote_copy(
        src_ref=view, dst_ref=view, send_sem=gram_send.at[0], recv_sem=gram_recv.at[0],
        device_id=(partner,), device_id_type=MESH,
    )
    gram_wait.wait_recv()
    full = jnp.sum(gram_in[...].astype(F32), axis=0).astype(BF16)
    blocks_p, offset = {}, 0
    for a in range(blocks):
        for b in range(a, blocks):
            piece = nn(full[:, offset:offset + block], orders[b].astype(BF16)).astype(BF16)
            blocks_p[a, b] = nn(places[a], piece).astype(BF16)
            offset += block

    lane = lax.broadcasted_iota(jnp.int32, (1, block), 1)
    sub = lax.broadcasted_iota(jnp.int32, (ROWS, block), 0)

    def times_gram(delta, piece):
        high = delta.astype(BF16).astype(F32)
        lhs = jnp.where(sub == 0, high, jnp.where(sub == 1, delta - high, 0.0)).astype(BF16)
        return 2.0 * jnp.sum(nn(lhs, piece)[0:8], axis=0, keepdims=True)

    def sweep(alpha, margin):
        result, margin = [], list(margin)
        for b in range(blocks):
            now, m, moved = alpha[b], margin[b], jnp.zeros((1, block), F32)
            for s in range(block // GROUP):
                fresh = jnp.clip(now + (1.0 - sign_p[b] * m) * inverse_p[b], 0.0, bound_p[b])
                mine = (lane >= s * GROUP) & (lane < (s + 1) * GROUP)
                change = jnp.where(mine, fresh - now, 0.0)
                now = jnp.where(mine, fresh, now)
                change = sign_p[b] * change
                moved = moved + change
                if s + 1 < block // GROUP:
                    m = m + times_gram(change, blocks_p[b, b])
            for later in range(b + 1, blocks):
                margin[later] = margin[later] + times_gram(moved, blocks_p[b, later])
            result.append(now)
        return result

    def changes(after, before):
        pieces = []
        for b in range(blocks):
            z = spread(sign_p[b] * (after[b] - before[b]))
            pieces.append(nt(z, orders[b].astype(BF16))[0:1, :])
        return jnp.concatenate(pieces, axis=1)

    one_p = sweep(zero_p, margin_p)
    own1[0:1, 0:rows] = changes(one_p, zero_p)
    own1[0:1, rows:] = jnp.broadcast_to(objective_part, (1, block))
    gather_start(own1, all1, 1 + 3)
    total_wait(all1, 4).wait_recv()
    update_one = back(all1) * (2.0 / devices)
    margin_parts(update_one, part2)
    scatter_start(part2, got2, 2)
    objective_ref[...] = jnp.sum(all1[...], axis=0)[:, rows:]
    total_wait(got2, 2).wait_recv()
    margin2 = margin1 + jnp.sum(got2[...], axis=0)
    margin2_p = [x[0:1] for x in permute((margin2,))]
    two_p = sweep(one_p, margin2_p)
    own2[...] = changes(two_p, one_p)
    gather_start(own2, all2, 2 + 3)
    for b in range(blocks):
        spot = jnp.broadcast_to(two_p[b], (8, block))
        alpha_ref[:, b * block:(b + 1) * block] = nt(spot, orders[b], HIGH)[0:1, :]
    total_wait(all2, 5).wait_recv()
    weight_ref[...] = primal + update_one + back(all2) * (2.0 / devices)

    for phase, ref in enumerate((got0, got1, got2)):
        total_wait(ref, phase).wait_send()
    for phase, ref in enumerate((all0, all1, all2)):
        total_wait(ref, phase + 3).wait_send()
    gram_wait.wait_send()

    def drain(c, carry):
        pair_copy(c).wait_send()
        return carry

    lax.fori_loop(0, chips, drain, 0)


def body(devices, data_t, labels, sample_weight, w_start, alpha_start, visit_order):
    me = lax.axis_index("shard")
    feats = data_t.shape[0]
    rows = alpha_start.shape[0]
    blocks, block = visit_order.shape
    chips = devices // 2
    width = sum(rows - a * block for a in range(blocks))
    sign = lax.dynamic_slice_in_dim(labels, me * rows, rows).astype(F32)[None]
    bound = lax.dynamic_slice_in_dim(sample_weight, me * rows, rows)[None]

    def vectors(height, length):
        return pltpu.VMEM((devices, height, length), F32)

    vmem = pl.BlockSpec(memory_space=pltpu.VMEM)
    weights, alpha, objective = pl.pallas_call(
        functools.partial(kernel, devices),
        name="svm_rounds",
        out_shape=(
            jax.ShapeDtypeStruct((1, feats), F32),
            jax.ShapeDtypeStruct((1, rows), F32),
            jax.ShapeDtypeStruct((1, block), F32),
        ),
        in_specs=[vmem] * 6,
        out_specs=(vmem,) * 3,
        scratch_shapes=[
            vectors(1, rows), vectors(2, rows), vectors(1, rows),
            vectors(1, rows), vectors(2, rows), vectors(1, rows),
            pltpu.VMEM((1, rows), F32), pltpu.VMEM((1, rows + block), F32), pltpu.VMEM((1, rows), F32),
            vectors(1, rows), vectors(1, rows + block), vectors(1, rows),
            pltpu.VMEM((devices, block, width), BF16),
            pltpu.VMEM((chips, block, width), BF16),
            pltpu.VMEM((chips, block, width), BF16),
            pltpu.VMEM((chips, block, width), BF16),
            pltpu.SemaphoreType.DMA((6,)),
            pltpu.SemaphoreType.DMA((6,)),
            pltpu.SemaphoreType.DMA((chips,)),
            pltpu.SemaphoreType.DMA((chips,)),
            pltpu.SemaphoreType.DMA((1,)),
            pltpu.SemaphoreType.DMA((1,)),
        ],
        compiler_params=pltpu.CompilerParams(
            collective_id=0, has_side_effects=True, vmem_limit_bytes=58 * 1024 * 1024
        ),
    )(data_t, sign, bound, w_start[None], alpha_start[None], visit_order)
    return weights[0], alpha[0], objective[0, 0]


def solution(mesh):
    placed = (P("shard", None), P(), P(), P("shard"), P("shard"), P("shard", None))
    return jax.shard_map(
        functools.partial(body, mesh.shape["shard"]), mesh=mesh, in_specs=placed,
        out_specs=(P("shard"), P("shard"), P()), check_vma=False,
    )
```

```python
import functools

import jax
import jax.numpy as jnp
from jax import lax
from jax.experimental import pallas as pl
from jax.experimental.pallas import tpu as pltpu
from jax.sharding import PartitionSpec as P

GROUP = 16
ROWS = 16
MESH = pl.DeviceIdType.MESH
F32 = jnp.float32
BF16 = jnp.bfloat16
HIGH = lax.Precision.HIGHEST


def nn(a, b, precision=None):
    return lax.dot_general(a, b, (((1,), (0,)), ((), ())), preferred_element_type=F32, precision=precision)


def nt(a, b, precision=None):
    return lax.dot_general(a, b, (((1,), (1,)), ((), ())), preferred_element_type=F32, precision=precision)


def spread(row):
    return jnp.broadcast_to(row, (ROWS, row.shape[-1])).astype(BF16)


def kernel(
    devices, data_ref, label_ref, bound_ref, start_ref, frac_ref, visit_ref,
    weight_ref, alpha_ref, objective_ref,
    part0, part1, part2, got0, got1, got2, own0, own1, own2, all0, all1, all2,
    gram, in_a, in_b, in_c, sum_a, sum_b, sum_c, gram_in,
    send_sem, recv_sem, send_a, recv_a, send_b, recv_b, send_c, recv_c, gram_send, gram_recv,
):
    me = lax.axis_index("shard")
    feats, samples = data_ref.shape
    rows = label_ref.shape[2]
    blocks, block = visit_ref.shape
    features = feats * devices
    cubes = devices // 8
    cube = me // 8
    bit0, bit1, bit2 = me % 2, (me // 2) % 2, (me // 4) % 2
    partner = me + 1 - 2 * bit0

    def columns(k):
        return pl.ds(pl.multiple_of(k * rows, rows), rows)

    def peers(action):
        def step(i, carry):
            action(lax.rem(me + i, devices))
            return carry

        lax.fori_loop(1, devices, step, 0)

    def total_wait(ref, phase):
        view = ref.at[pl.ds(0, devices - 1)]
        return pltpu.make_async_remote_copy(
            src_ref=view, dst_ref=view, send_sem=send_sem.at[phase], recv_sem=recv_sem.at[phase],
            device_id=(partner,), device_id_type=MESH,
        )

    def scatter_start(part, got, phase):
        def send(peer):
            pltpu.make_async_remote_copy(
                src_ref=part.at[peer], dst_ref=got.at[me], send_sem=send_sem.at[phase],
                recv_sem=recv_sem.at[phase], device_id=(peer,), device_id_type=MESH,
            ).start()

        peers(send)
        got[me] = part[me]

    def gather_start(own, everyone, phase):
        def send(peer):
            pltpu.make_async_remote_copy(
                src_ref=own, dst_ref=everyone.at[me], send_sem=send_sem.at[phase],
                recv_sem=recv_sem.at[phase], device_id=(peer,), device_id_type=MESH,
            ).start()

        peers(send)
        everyone[me] = own[...]

    def margin_parts(row, part):
        lhs = spread(row)

        def step(k, carry):
            part[k, 0:1, :] = nn(lhs, data_ref[:, columns(k)])[0:1, :]
            return carry

        lax.fori_loop(0, devices, step, 0, unroll=4)

    def back(everyone):
        def step(k, total):
            return total + nt(spread(everyone[k][0:1, 0:rows]), data_ref[:, columns(k)])

        return lax.fori_loop(0, devices, step, jnp.zeros((ROWS, feats), F32), unroll=4)[0:1, :]

    barrier = pltpu.get_barrier_semaphore()
    peers(lambda peer: pl.semaphore_signal(barrier, inc=1, device_id=(peer,), device_id_type=MESH))

    w_start = start_ref[...]
    sign, bound = label_ref[me].astype(F32), bound_ref[me]
    margin_parts(w_start, part0)
    pl.semaphore_wait(barrier, devices - 1)
    scatter_start(part0, got0, 0)

    row_at = lax.broadcasted_iota(jnp.int32, (block, block), 0)
    lane_at = lax.broadcasted_iota(jnp.int32, (block, block), 1)
    upper, lower = row_at < lane_at, row_at > lane_at

    def gram_of(k):
        tile = data_ref[:, columns(k)]
        first, second = tile[:, :block], tile[:, block:]
        top = lax.dot_general(first, tile, (((0,), (0,)), ((), ())), preferred_element_type=F32)
        low = lax.dot_general(second, second, (((0,), (0,)), ((), ())), preferred_element_type=F32)
        gram[k, :, :block] = jnp.where(upper, top[:, :block], low).astype(BF16)
        gram[k, :, block:] = top[:, block:].astype(BF16)
        square = tile.astype(F32)
        square = square * square
        part1[k, 1:2, :] = jnp.sum(square, axis=0, keepdims=True)
        return square

    def halving(source, target, index, sends, recvs, peer):
        return pltpu.make_async_remote_copy(
            src_ref=source, dst_ref=target.at[index], send_sem=sends.at[index],
            recv_sem=recvs.at[index], device_id=(peer,), device_id_type=MESH,
        )

    def copy_a(q, j):
        return halving(gram.at[8 * q + 2 * j + 1 - bit0], in_a, 4 * q + j, send_a, recv_a, partner)

    def copy_b(q, j):
        return halving(sum_a.at[4 * q + 2 * j + 1 - bit1], in_b, 2 * q + j, send_b, recv_b, me + 2 - 4 * bit1)

    def copy_c(q):
        return halving(sum_b.at[2 * q + 1 - bit2], in_c, q, send_c, recv_c, me + 4 - 8 * bit2)

    def copy_d(q):
        return pltpu.make_async_remote_copy(
            src_ref=sum_c.at[q], dst_ref=gram_in.at[cube], send_sem=gram_send.at[0],
            recv_sem=gram_recv.at[0], device_id=(me + 8 * (q - cube),), device_id_type=MESH,
        )

    def added(x, y):
        return (x.astype(F32) + y.astype(F32)).astype(BF16)

    def turn(i):
        return lax.rem(cube + 1 + i, cubes)

    def merge_a(i):
        q = turn(i)
        for j in range(2):
            j = (j + 1 + bit2) % 2
            for side in (1 - bit1, bit1):
                at = 2 * j + side
                copy_a(q, at).wait_recv()
                sum_a[4 * q + at] = added(gram[8 * q + 2 * at + bit0], in_a[4 * q + at])
            copy_b(q, j).start()

    def merge_b(i):
        q = turn(i)
        for j in (1 - bit2, bit2):
            copy_b(q, j).wait_recv()
            sum_b[2 * q + j] = added(sum_a[4 * q + 2 * j + bit1], in_b[2 * q + j])
        copy_c(q).start()

    def merged_c(q):
        copy_c(q).wait_recv()
        return added(sum_b[2 * q + bit2], in_c[q])

    def merge_c(i):
        q = turn(i)
        sum_c[q] = merged_c(q)
        copy_d(q).start()

    def loop(count, action):
        def step(i, carry):
            action(i)
            return carry

        lax.fori_loop(0, count, step, 0)

    def gram_step(i, total):
        q = turn(i)
        for j in range(4):
            total = total + gram_of(8 * q + 2 * j + 1 - bit0)
            copy_a(q, j).start()
        for j in range(4):
            total = total + gram_of(8 * q + 2 * j + bit0)
        merge_a(i)
        return total

    square_total = lax.fori_loop(0, cubes, gram_step, jnp.zeros((feats, rows), F32))
    column_sq = nt(jnp.ones((8, rows), F32), square_total, HIGH)[0:1, :]

    total_wait(got0, 0).wait_recv()
    margin0 = jnp.sum(got0[...], axis=0)
    own0[...] = bound * sign * jnp.maximum(0.0, 1.0 - sign * margin0)
    gather_start(own0, all0, 0 + 3)

    loop(cubes, merge_b)

    total_wait(all0, 3).wait_recv()
    ascent = back(all0)
    loop(cubes - 1, merge_c)
    gram_in[cube] = merged_c(cube)
    scale = column_sq / samples + 1e-06
    stepped = w_start + ascent / (samples * scale)
    thresh = 1.0 / (4.0 * features * scale)
    primal = stepped - jnp.clip(stepped, -thresh, thresh)
    margin_parts(primal, part1)
    scatter_start(part1, got1, 1)

    orders, places = [], []
    for b in range(blocks):
        order = (lax.broadcasted_iota(jnp.int32, (block, block), 0) == visit_ref[b:b + 1, :]).astype(F32)
        orders.append(order)
        places.append(order.T.astype(BF16))

    alpha_zero = bound * frac_ref[...]

    def permute(vectors):
        stacked = jnp.concatenate(list(vectors) + [jnp.zeros((8 - len(vectors), rows), F32)], axis=0)
        return [nn(stacked[:, b * block:(b + 1) * block], orders[b], HIGH) for b in range(blocks)]

    total_wait(got1, 1).wait_recv()
    received = jnp.sum(got1[...], axis=0)
    margin1, diag = received[0:1, :], received[1:2, :]
    loss = jnp.sum(bound * jnp.square(jnp.maximum(0.0, 1.0 - sign * margin1)), axis=1, keepdims=True)
    penalty = jnp.sum(jnp.abs(primal), axis=1, keepdims=True)
    objective_part = loss / (2.0 * samples) + penalty / (4.0 * features)
    permuted = permute((sign, bound, alpha_zero, diag, margin1))
    sign_p = [x[0:1] for x in permuted]
    bound_p = [x[1:2] for x in permuted]
    zero_p = [x[2:3] for x in permuted]
    inverse_p = [0.5 / (x[3:4] + 1e-06) for x in permuted]
    margin_p = [x[4:5] for x in permuted]

    view = gram_in.at[pl.ds(0, cubes - 1)]
    gram_wait = pltpu.make_async_remote_copy(
        src_ref=view, dst_ref=view, send_sem=gram_send.at[0], recv_sem=gram_recv.at[0],
        device_id=(partner,), device_id_type=MESH,
    )
    gram_wait.wait_recv()
    full = jnp.sum(gram_in[...].astype(F32), axis=0)
    packed, cross = full[:, :block], full[:, block:]
    above, below = jnp.where(upper, packed, 0.0), jnp.where(lower, packed, 0.0)
    blocks_p = {}
    for (a, b), piece in {(0, 0): above + above.T, (0, 1): cross, (1, 1): below + below.T}.items():
        piece = nn(piece.astype(BF16), orders[b].astype(BF16)).astype(BF16)
        blocks_p[a, b] = nn(places[a], piece).astype(BF16)

    lane = lax.broadcasted_iota(jnp.int32, (1, block), 1)
    sub = lax.broadcasted_iota(jnp.int32, (ROWS, block), 0)

    def times_gram(delta, piece):
        high = delta.astype(BF16).astype(F32)
        lhs = jnp.where(sub == 0, high, jnp.where(sub == 1, delta - high, 0.0)).astype(BF16)
        return 2.0 * jnp.sum(nn(lhs, piece)[0:8], axis=0, keepdims=True)

    def sweep(alpha, margin):
        result, margin = [], list(margin)
        for b in range(blocks):
            now, m, moved = alpha[b], margin[b], jnp.zeros((1, block), F32)
            for s in range(block // GROUP):
                fresh = jnp.clip(now + (1.0 - sign_p[b] * m) * inverse_p[b], 0.0, bound_p[b])
                mine = (lane >= s * GROUP) & (lane < (s + 1) * GROUP)
                change = jnp.where(mine, fresh - now, 0.0)
                now = jnp.where(mine, fresh, now)
                change = sign_p[b] * change
                moved = moved + change
                if s + 1 < block // GROUP:
                    m = m + times_gram(change, blocks_p[b, b])
            for later in range(b + 1, blocks):
                margin[later] = margin[later] + times_gram(moved, blocks_p[b, later])
            result.append(now)
        return result

    def changes(after, before):
        pieces = []
        for b in range(blocks):
            z = spread(sign_p[b] * (after[b] - before[b]))
            pieces.append(nt(z, orders[b].astype(BF16))[0:1, :])
        return jnp.concatenate(pieces, axis=1)

    one_p = sweep(zero_p, margin_p)
    own1[0:1, 0:rows] = changes(one_p, zero_p)
    own1[0:1, rows:] = jnp.broadcast_to(objective_part, (1, block))
    gather_start(own1, all1, 1 + 3)
    total_wait(all1, 4).wait_recv()
    update_one = back(all1) * (2.0 / devices)
    margin_parts(update_one, part2)
    scatter_start(part2, got2, 2)
    objective_ref[...] = jnp.sum(all1[...], axis=0)[:, rows:]
    total_wait(got2, 2).wait_recv()
    margin2 = margin1 + jnp.sum(got2[...], axis=0)
    margin2_p = [x[0:1] for x in permute((margin2,))]
    two_p = sweep(one_p, margin2_p)
    own2[...] = changes(two_p, one_p)
    gather_start(own2, all2, 2 + 3)
    for b in range(blocks):
        spot = jnp.broadcast_to(two_p[b], (8, block))
        alpha_ref[:, b * block:(b + 1) * block] = nt(spot, orders[b], HIGH)[0:1, :]
    total_wait(all2, 5).wait_recv()
    weight_ref[...] = primal + update_one + back(all2) * (2.0 / devices)

    for phase, ref in enumerate((got0, got1, got2)):
        total_wait(ref, phase).wait_send()
    for phase, ref in enumerate((all0, all1, all2)):
        total_wait(ref, phase + 3).wait_send()
    gram_wait.wait_send()

    def drain(q):
        for j in range(4):
            copy_a(q, j).wait_send()
        for j in range(2):
            copy_b(q, j).wait_send()
        copy_c(q).wait_send()

    loop(cubes, drain)


def body(devices, data_t, labels, sample_weight, w_start, alpha_start, visit_order):
    feats = data_t.shape[0]
    rows = alpha_start.shape[0]
    blocks, block = visit_order.shape
    cubes = devices // 8
    labels = labels.reshape(devices, 1, rows)
    bound = sample_weight.reshape(devices, 1, rows)

    def grams(count):
        return pltpu.VMEM((count, block, rows), BF16)

    def semaphores(count):
        return pltpu.SemaphoreType.DMA((count,))

    def vectors(height, length):
        return pltpu.VMEM((devices, height, length), F32)

    vmem = pl.BlockSpec(memory_space=pltpu.VMEM)
    weights, alpha, objective = pl.pallas_call(
        functools.partial(kernel, devices),
        name="svm_rounds",
        out_shape=(
            jax.ShapeDtypeStruct((1, feats), F32),
            jax.ShapeDtypeStruct((1, rows), F32),
            jax.ShapeDtypeStruct((1, block), F32),
        ),
        in_specs=[vmem] * 6,
        out_specs=(vmem,) * 3,
        scratch_shapes=[
            vectors(1, rows), vectors(2, rows), vectors(1, rows),
            vectors(1, rows), vectors(2, rows), vectors(1, rows),
            pltpu.VMEM((1, rows), F32), pltpu.VMEM((1, rows + block), F32), pltpu.VMEM((1, rows), F32),
            vectors(1, rows), vectors(1, rows + block), vectors(1, rows),
            grams(devices), grams(4 * cubes), grams(2 * cubes), grams(cubes),
            grams(4 * cubes), grams(2 * cubes), grams(cubes), grams(cubes),
            semaphores(6), semaphores(6), semaphores(4 * cubes), semaphores(4 * cubes),
            semaphores(2 * cubes), semaphores(2 * cubes), semaphores(cubes), semaphores(cubes),
            semaphores(1), semaphores(1),
        ],
        compiler_params=pltpu.CompilerParams(
            collective_id=0, has_side_effects=True, vmem_limit_bytes=58 * 1024 * 1024
        ),
    )(data_t, labels, bound, w_start[None], alpha_start[None], visit_order)
    return weights[0], alpha[0], objective[0, 0]


def solution(mesh):
    placed = (P("shard", None), P(), P(), P("shard"), P("shard"), P("shard", None))
    return jax.shard_map(
        functools.partial(body, mesh.shape["shard"]), mesh=mesh, in_specs=placed,
        out_specs=(P("shard"), P("shard"), P()), check_vma=False,
    )
```

```python
import functools

import jax
import jax.numpy as jnp
from jax import lax
from jax.experimental import pallas as pl
from jax.experimental.pallas import tpu as pltpu
from jax.sharding import PartitionSpec as P

GROUP = 16
ROWS = 16
MESH = pl.DeviceIdType.MESH
F32 = jnp.float32
BF16 = jnp.bfloat16
HIGH = lax.Precision.HIGHEST


def nn(a, b, precision=None):
    return lax.dot_general(a, b, (((1,), (0,)), ((), ())), preferred_element_type=F32, precision=precision)


def nt(a, b, precision=None):
    return lax.dot_general(a, b, (((1,), (1,)), ((), ())), preferred_element_type=F32, precision=precision)


def spread(row):
    return jnp.broadcast_to(row, (ROWS, row.shape[-1])).astype(BF16)


def kernel(
    devices, data_hbm, label_ref, bound_ref, start_ref, frac_ref, visit_ref,
    weight_ref, alpha_ref, objective_ref,
    part0, part1, part2, got0, got1, got2, own0, own1, own2, all0, all1, all2,
    data_ref, gram, in_a, in_b, in_c, sum_a, sum_b, sum_c, gram_in,
    load_sem, send_sem, recv_sem, gather_sem, send_a, recv_a, send_b, recv_b, send_c, recv_c, gram_send, gram_recv,
):
    me = lax.axis_index("shard")
    feats, samples = data_hbm.shape
    rows = label_ref.shape[2]
    blocks, block = visit_ref.shape
    features = feats * devices
    cubes = devices // 8
    cube = me // 8
    bit0, bit1, bit2 = me % 2, (me // 2) % 2, (me // 4) % 2
    partner = me + 1 - 2 * bit0

    def columns(k):
        return pl.ds(pl.multiple_of(k * rows, rows), rows)

    def loop(first, last, action):
        def step(i, carry):
            action(i)
            return carry

        lax.fori_loop(first, last, step, 0)

    upward = cube // (cubes // 2)

    def near(i):
        place = upward * (cubes - 2 - i) + (1 - upward) * i
        return place + jnp.where(place >= cube, 1, 0)

    def far(i):
        return near(cubes - 2 - i)

    def mates(action):
        loop(1, 8, lambda i: action(8 * cube + lax.rem(me + i, 8)))

    def cube_of(q, action):
        loop(0, 8, lambda j: action(8 * q + j))

    def peers(action):
        loop(0, cubes - 1, lambda i: cube_of(far(i), action))
        mates(action)

    def remote(source, target, send, recv, peer):
        return pltpu.make_async_remote_copy(
            src_ref=source, dst_ref=target, send_sem=send, recv_sem=recv,
            device_id=(peer,), device_id_type=MESH,
        )

    def total_wait(ref, phase):
        view = ref.at[pl.ds(0, devices - 1)]
        return remote(view, view, send_sem.at[phase], recv_sem.at[phase % 3], partner)

    def scatter_send(part, got, phase):
        def send(peer):
            remote(part.at[peer], got.at[me], send_sem.at[phase], recv_sem.at[phase], peer).start()

        return send

    def gather_start(own, everyone, phase):
        everyone[me] = own[...]
        spot = (phase - 3) * cubes + cube
        peers(lambda peer: remote(own, everyone.at[me], send_sem.at[phase], gather_sem.at[spot], peer).start())

    def part_of(lhs, part, q):
        for j in range(8):
            k = 8 * q + j
            part[k, 0:1, :] = nn(lhs, data_ref[:, columns(k)])[0:1, :]

    def margin_scatter(row, part, got, phase):
        lhs = spread(row)
        send = scatter_send(part, got, phase)

        def step(i):
            q = far(i)
            part_of(lhs, part, q)
            cube_of(q, send)

        loop(0, cubes - 1, step)
        part_of(lhs, part, cube)
        mates(send)
        got[me] = part[me]

    def back(everyone, phase):
        def arrival(q, count):
            view = everyone.at[pl.ds(8 * q, count)]
            spot = (phase - 3) * cubes + q
            remote(view, view, send_sem.at[phase], gather_sem.at[spot], partner).wait_recv()

        def cube_sum(q, total):
            for j in range(8):
                k = 8 * q + j
                total = total + nt(spread(everyone[k][0:1, 0:rows]), data_ref[:, columns(k)])
            return total

        def step(i, total):
            q = near(i)
            arrival(q, 8)
            return cube_sum(q, total)

        arrival(cube, 7)
        total = cube_sum(cube, jnp.zeros((ROWS, feats), F32))
        return lax.fori_loop(0, cubes - 1, step, total)[0:1, :]

    def load(q):
        view = pl.ds(pl.multiple_of(8 * q * rows, rows), 8 * rows)
        return pltpu.make_async_copy(data_hbm.at[:, view], data_ref.at[:, view], load_sem.at[q])

    loop(0, cubes - 1, lambda i: load(far(i)).start())
    load(cube).start()
    barrier = pltpu.get_barrier_semaphore()
    peers(lambda peer: pl.semaphore_signal(barrier, inc=1, device_id=(peer,), device_id_type=MESH))

    w_start = start_ref[...]
    sign, bound = label_ref[me].astype(F32), bound_ref[me]
    start_rows = spread(w_start)

    def first_part(q):
        load(q).wait()
        part_of(start_rows, part0, q)

    loop(0, cubes - 1, lambda i: first_part(far(i)))
    first_part(cube)
    pl.semaphore_wait(barrier, devices - 1)
    peers(scatter_send(part0, got0, 0))
    got0[me] = part0[me]

    row_at = lax.broadcasted_iota(jnp.int32, (block, block), 0)
    lane_at = lax.broadcasted_iota(jnp.int32, (block, block), 1)
    upper, lower = row_at < lane_at, row_at > lane_at

    def gram_of(k):
        tile = data_ref[:, columns(k)]
        first, second = tile[:, :block], tile[:, block:]
        top = lax.dot_general(first, tile, (((0,), (0,)), ((), ())), preferred_element_type=F32)
        low = lax.dot_general(second, second, (((0,), (0,)), ((), ())), preferred_element_type=F32)
        gram[k, :, :block] = jnp.where(upper, top[:, :block], low).astype(BF16)
        gram[k, :, block:] = top[:, block:].astype(BF16)
        square = tile.astype(F32)
        square = square * square
        part1[k, 1:2, :] = jnp.sum(square, axis=0, keepdims=True)
        return square

    def halving(source, target, index, sends, recvs, peer):
        return pltpu.make_async_remote_copy(
            src_ref=source, dst_ref=target.at[index], send_sem=sends.at[index],
            recv_sem=recvs.at[index], device_id=(peer,), device_id_type=MESH,
        )

    def copy_a(q, j):
        return halving(gram.at[8 * q + 2 * j + 1 - bit0], in_a, 4 * q + j, send_a, recv_a, partner)

    def order_of(q):
        swap = q % 2
        return (1 - swap) * bit1 + swap * bit2, 1 + swap, (1 - swap) * bit2 + swap * bit1, 2 - swap

    def copy_b(q, t):
        bit, weight, _, other = order_of(q)
        return halving(
            sum_a.at[4 * q + weight * (1 - bit) + other * t], in_b, 2 * q + t, send_b, recv_b,
            me + 2 * weight * (1 - 2 * bit),
        )

    def copy_c(q):
        _, _, bit, weight = order_of(q)
        return halving(sum_b.at[2 * q + 1 - bit], in_c, q, send_c, recv_c, me + 2 * weight * (1 - 2 * bit))

    def copy_d(q):
        return pltpu.make_async_remote_copy(
            src_ref=sum_c.at[q], dst_ref=gram_in.at[cube], send_sem=gram_send.at[0],
            recv_sem=gram_recv.at[0], device_id=(me + 8 * (q - cube),), device_id_type=MESH,
        )

    def added(x, y):
        return (x.astype(F32) + y.astype(F32)).astype(BF16)

    def turn(i):
        return lax.rem(cube + 1 + i, cubes)

    def merge_a(i):
        q = turn(i)
        bit, weight, last, other = order_of(q)
        for t in (1 - last, last):
            for side in (1 - bit, bit):
                at = weight * side + other * t
                copy_a(q, at).wait_recv()
                sum_a[4 * q + at] = added(gram[8 * q + 2 * at + bit0], in_a[4 * q + at])
            copy_b(q, t).start()

    def merge_b(i):
        q = turn(i)
        bit, weight, last, other = order_of(q)
        for t in (1 - last, last):
            copy_b(q, t).wait_recv()
            sum_b[2 * q + t] = added(sum_a[4 * q + weight * bit + other * t], in_b[2 * q + t])
        copy_c(q).start()

    def merged_c(q):
        bit = order_of(q)[2]
        copy_c(q).wait_recv()
        return added(sum_b[2 * q + bit], in_c[q])

    def merge_c(i):
        q = turn(i)
        sum_c[q] = merged_c(q)
        copy_d(q).start()

    def gram_step(i, total):
        q = turn(i)
        for j in range(4):
            total = total + gram_of(8 * q + 2 * j + 1 - bit0)
            copy_a(q, j).start()
        for j in range(4):
            total = total + gram_of(8 * q + 2 * j + bit0)
        merge_a(i)
        return total

    half = cubes // 2
    square_total = lax.fori_loop(0, half, gram_step, jnp.zeros((feats, rows), F32))
    total_wait(got0, 0).wait_recv()
    margin0 = jnp.sum(got0[...], axis=0)
    own0[...] = bound * sign * jnp.maximum(0.0, 1.0 - sign * margin0)
    gather_start(own0, all0, 0 + 3)

    def late_step(i, total):
        total = gram_step(i, total)
        merge_b(i - half)
        return total

    square_total = lax.fori_loop(half, cubes, late_step, square_total)
    column_sq = nt(jnp.ones((8, rows), F32), square_total, HIGH)[0:1, :]
    ascent = back(all0, 3)
    loop(cubes - half, cubes - 1, merge_b)
    scale = column_sq / samples + 1e-06
    stepped = w_start + ascent / (samples * scale)
    thresh = 1.0 / (4.0 * features * scale)
    primal = stepped - jnp.clip(stepped, -thresh, thresh)
    margin_scatter(primal, part1, got1, 1)
    merge_b(cubes - 1)
    loop(0, cubes - 1, merge_c)
    gram_in[cube] = merged_c(cube)

    orders, places = [], []
    for b in range(blocks):
        order = (lax.broadcasted_iota(jnp.int32, (block, block), 0) == visit_ref[b:b + 1, :]).astype(F32)
        orders.append(order)
        places.append(order.T.astype(BF16))

    alpha_zero = bound * frac_ref[...]

    def permute(vectors):
        stacked = jnp.concatenate(list(vectors) + [jnp.zeros((8 - len(vectors), rows), F32)], axis=0)
        return [nn(stacked[:, b * block:(b + 1) * block], orders[b], HIGH) for b in range(blocks)]

    total_wait(got1, 1).wait_recv()
    received = jnp.sum(got1[...], axis=0)
    margin1, diag = received[0:1, :], received[1:2, :]
    loss = jnp.sum(bound * jnp.square(jnp.maximum(0.0, 1.0 - sign * margin1)), axis=1, keepdims=True)
    penalty = jnp.sum(jnp.abs(primal), axis=1, keepdims=True)
    objective_part = loss / (2.0 * samples) + penalty / (4.0 * features)
    permuted = permute((sign, bound, alpha_zero, diag, margin1))
    sign_p = [x[0:1] for x in permuted]
    bound_p = [x[1:2] for x in permuted]
    zero_p = [x[2:3] for x in permuted]
    inverse_p = [0.5 / (x[3:4] + 1e-06) for x in permuted]
    margin_p = [x[4:5] for x in permuted]

    view = gram_in.at[pl.ds(0, cubes - 1)]
    gram_wait = pltpu.make_async_remote_copy(
        src_ref=view, dst_ref=view, send_sem=gram_send.at[0], recv_sem=gram_recv.at[0],
        device_id=(partner,), device_id_type=MESH,
    )
    gram_wait.wait_recv()
    full = jnp.sum(gram_in[...].astype(F32), axis=0)
    packed, cross = full[:, :block], full[:, block:]
    above, below = jnp.where(upper, packed, 0.0), jnp.where(lower, packed, 0.0)
    blocks_p = {}
    for (a, b), piece in {(0, 0): above + above.T, (0, 1): cross, (1, 1): below + below.T}.items():
        piece = nn(piece.astype(BF16), orders[b].astype(BF16)).astype(BF16)
        blocks_p[a, b] = nn(places[a], piece).astype(BF16)

    lane = lax.broadcasted_iota(jnp.int32, (1, block), 1)
    sub = lax.broadcasted_iota(jnp.int32, (ROWS, block), 0)

    def times_gram(delta, piece):
        high = delta.astype(BF16).astype(F32)
        lhs = jnp.where(sub == 0, high, jnp.where(sub == 1, delta - high, 0.0)).astype(BF16)
        return 2.0 * jnp.sum(nn(lhs, piece)[0:8], axis=0, keepdims=True)

    def sweep(alpha, margin):
        result, margin = [], list(margin)
        for b in range(blocks):
            now, m, moved = alpha[b], margin[b], jnp.zeros((1, block), F32)
            for s in range(block // GROUP):
                fresh = jnp.clip(now + (1.0 - sign_p[b] * m) * inverse_p[b], 0.0, bound_p[b])
                mine = (lane >= s * GROUP) & (lane < (s + 1) * GROUP)
                change = jnp.where(mine, fresh - now, 0.0)
                now = jnp.where(mine, fresh, now)
                change = sign_p[b] * change
                moved = moved + change
                if s + 1 < block // GROUP:
                    m = m + times_gram(change, blocks_p[b, b])
            for later in range(b + 1, blocks):
                margin[later] = margin[later] + times_gram(moved, blocks_p[b, later])
            result.append(now)
        return result

    def changes(after, before):
        pieces = []
        for b in range(blocks):
            z = spread(sign_p[b] * (after[b] - before[b]))
            pieces.append(nt(z, orders[b].astype(BF16))[0:1, :])
        return jnp.concatenate(pieces, axis=1)

    one_p = sweep(zero_p, margin_p)
    own1[0:1, 0:rows] = changes(one_p, zero_p)
    own1[0:1, rows:] = jnp.broadcast_to(objective_part, (1, block))
    gather_start(own1, all1, 1 + 3)
    update_one = back(all1, 4) * (2.0 / devices)
    margin_scatter(update_one, part2, got2, 2)
    objective_ref[...] = jnp.sum(all1[...], axis=0)[:, rows:]
    total_wait(got2, 2).wait_recv()
    margin2 = margin1 + jnp.sum(got2[...], axis=0)
    margin2_p = [x[0:1] for x in permute((margin2,))]
    two_p = sweep(one_p, margin2_p)
    own2[...] = changes(two_p, one_p)
    gather_start(own2, all2, 2 + 3)
    for b in range(blocks):
        spot = jnp.broadcast_to(two_p[b], (8, block))
        alpha_ref[:, b * block:(b + 1) * block] = nt(spot, orders[b], HIGH)[0:1, :]
    weight_ref[...] = primal + update_one + back(all2, 5) * (2.0 / devices)

    for phase, ref in enumerate((got0, got1, got2)):
        total_wait(ref, phase).wait_send()
    for phase, ref in enumerate((all0, all1, all2)):
        total_wait(ref, phase + 3).wait_send()
    gram_wait.wait_send()

    def drain(q):
        for j in range(4):
            copy_a(q, j).wait_send()
        for j in range(2):
            copy_b(q, j).wait_send()
        copy_c(q).wait_send()

    loop(0, cubes, drain)


def body(devices, data_t, labels, sample_weight, w_start, alpha_start, visit_order):
    feats = data_t.shape[0]
    rows = alpha_start.shape[0]
    blocks, block = visit_order.shape
    cubes = devices // 8
    labels = labels.reshape(devices, 1, rows)
    bound = sample_weight.reshape(devices, 1, rows)

    def grams(count):
        return pltpu.VMEM((count, block, rows), BF16)

    def semaphores(count):
        return pltpu.SemaphoreType.DMA((count,))

    def vectors(height, length):
        return pltpu.VMEM((devices, height, length), F32)

    vmem = pl.BlockSpec(memory_space=pltpu.VMEM)
    weights, alpha, objective = pl.pallas_call(
        functools.partial(kernel, devices),
        name="svm_rounds",
        out_shape=(
            jax.ShapeDtypeStruct((1, feats), F32),
            jax.ShapeDtypeStruct((1, rows), F32),
            jax.ShapeDtypeStruct((1, block), F32),
        ),
        in_specs=[pl.BlockSpec(memory_space=pl.ANY)] + [vmem] * 5,
        out_specs=(vmem,) * 3,
        scratch_shapes=[
            vectors(1, rows), vectors(2, rows), vectors(1, rows),
            vectors(1, rows), vectors(2, rows), vectors(1, rows),
            pltpu.VMEM((1, rows), F32), pltpu.VMEM((1, rows + block), F32), pltpu.VMEM((1, rows), F32),
            vectors(1, rows), vectors(1, rows + block), vectors(1, rows),
            pltpu.VMEM(data_t.shape, BF16), grams(devices), grams(4 * cubes), grams(2 * cubes), grams(cubes),
            grams(4 * cubes), grams(2 * cubes), grams(cubes), grams(cubes),
            semaphores(cubes), semaphores(6), semaphores(3), semaphores(3 * cubes), semaphores(4 * cubes), semaphores(4 * cubes),
            semaphores(2 * cubes), semaphores(2 * cubes), semaphores(cubes), semaphores(cubes),
            semaphores(1), semaphores(1),
        ],
        compiler_params=pltpu.CompilerParams(
            collective_id=0, has_side_effects=True, vmem_limit_bytes=63 * 1024 * 1024
        ),
    )(data_t, labels, bound, w_start[None], alpha_start[None], visit_order)
    return weights[0], alpha[0], objective[0, 0]


def solution(mesh):
    placed = (P("shard", None), P(), P(), P("shard"), P("shard"), P("shard", None))
    return jax.shard_map(
        functools.partial(body, mesh.shape["shard"]), mesh=mesh, in_specs=placed,
        out_specs=(P("shard"), P("shard"), P()), check_vma=False,
    )
```

```python
import functools

import jax
import jax.numpy as jnp
from jax import lax
from jax.experimental import pallas as pl
from jax.experimental.pallas import tpu as pltpu
from jax.sharding import PartitionSpec as P

GROUP = 16
ROWS = 16
MESH = pl.DeviceIdType.MESH
F32 = jnp.float32
BF16 = jnp.bfloat16
HIGH = lax.Precision.HIGHEST


def nn(a, b, precision=None):
    return lax.dot_general(a, b, (((1,), (0,)), ((), ())), preferred_element_type=F32, precision=precision)


def nt(a, b, precision=None):
    return lax.dot_general(a, b, (((1,), (1,)), ((), ())), preferred_element_type=F32, precision=precision)


def spread(row):
    return jnp.broadcast_to(row, (ROWS, row.shape[-1])).astype(BF16)


def kernel(
    devices, data_hbm, label_ref, bound_ref, start_ref, frac_ref, visit_ref,
    out_ref,
    part0, part1, part2, got0, got1, got2, own0, own1, own2, all0, all1, all2,
    data_ref, gram, in_a, in_b, in_c, sum_a, sum_b, sum_c, gram_in,
    load_sem, send_sem, recv_sem, gather_sem, send_a, recv_a, send_b, recv_b, send_c, recv_c, gram_send, gram_recv,
):
    me = lax.axis_index("shard")
    feats, samples = data_hbm.shape
    rows = label_ref.shape[2]
    blocks, block = visit_ref.shape
    features = feats * devices
    cubes = devices // 8
    cube = me // 8
    bit0, bit1, bit2 = me % 2, (me // 2) % 2, (me // 4) % 2
    partner = me + 1 - 2 * bit0

    def columns(k):
        return pl.ds(pl.multiple_of(k * rows, rows), rows)

    def loop(first, last, action):
        def step(i, carry):
            action(i)
            return carry

        lax.fori_loop(first, last, step, 0)

    upward = cube // (cubes // 2)

    def near(i):
        place = upward * (cubes - 2 - i) + (1 - upward) * i
        return place + jnp.where(place >= cube, 1, 0)

    def far(i):
        return near(cubes - 2 - i)

    def mates(action):
        loop(1, 8, lambda i: action(8 * cube + lax.rem(me + i, 8)))

    def cube_of(q, action):
        loop(0, 8, lambda j: action(8 * q + j))

    def peers(action):
        loop(0, cubes - 1, lambda i: cube_of(far(i), action))
        mates(action)

    def remote(source, target, send, recv, peer):
        return pltpu.make_async_remote_copy(
            src_ref=source, dst_ref=target, send_sem=send, recv_sem=recv,
            device_id=(peer,), device_id_type=MESH,
        )

    def total_wait(ref, phase):
        view = ref.at[pl.ds(0, devices - 1)]
        return remote(view, view, send_sem.at[phase], recv_sem.at[phase % 3], partner)

    def scatter_send(part, got, phase):
        def send(peer):
            remote(part.at[peer], got.at[me], send_sem.at[phase], recv_sem.at[phase], peer).start()

        return send

    def gather_start(own, everyone, phase):
        everyone[me] = own[...]
        spot = (phase - 3) * cubes + cube
        peers(lambda peer: remote(own, everyone.at[me], send_sem.at[phase], gather_sem.at[spot], peer).start())

    def part_of(lhs, part, q):
        for j in range(8):
            k = 8 * q + j
            part[k, 0:1, :] = nn(lhs, data_ref[:, columns(k)])[0:1, :]

    def margin_scatter(row, part, got, phase):
        lhs = spread(row)
        send = scatter_send(part, got, phase)

        def step(i):
            q = far(i)
            part_of(lhs, part, q)
            cube_of(q, send)

        loop(0, cubes - 1, step)
        part_of(lhs, part, cube)
        mates(send)
        got[me] = part[me]

    def back(everyone, phase):
        def arrival(q, count):
            view = everyone.at[pl.ds(8 * q, count)]
            spot = (phase - 3) * cubes + q
            remote(view, view, send_sem.at[phase], gather_sem.at[spot], partner).wait_recv()

        def cube_sum(q, total):
            for j in range(8):
                k = 8 * q + j
                total = total + nt(spread(everyone[k][0:1, 0:rows]), data_ref[:, columns(k)])
            return total

        def step(i, total):
            q = near(i)
            arrival(q, 8)
            return cube_sum(q, total)

        arrival(cube, 7)
        total = cube_sum(cube, jnp.zeros((ROWS, feats), F32))
        return lax.fori_loop(0, cubes - 1, step, total)[0:1, :]

    def load(q):
        view = pl.ds(pl.multiple_of(8 * q * rows, rows), 8 * rows)
        return pltpu.make_async_copy(data_hbm.at[:, view], data_ref.at[:, view], load_sem.at[q])

    loop(0, cubes - 1, lambda i: load(far(i)).start())
    load(cube).start()
    barrier = pltpu.get_barrier_semaphore()
    peers(lambda peer: pl.semaphore_signal(barrier, inc=1, device_id=(peer,), device_id_type=MESH))

    w_start = start_ref[...]
    sign, bound = label_ref[me].astype(F32), bound_ref[me]
    start_rows = spread(w_start)

    def first_part(q):
        load(q).wait()
        part_of(start_rows, part0, q)

    loop(0, cubes - 1, lambda i: first_part(far(i)))
    first_part(cube)
    pl.semaphore_wait(barrier, devices - 1)
    peers(scatter_send(part0, got0, 0))
    got0[me] = part0[me]

    row_at = lax.broadcasted_iota(jnp.int32, (block, block), 0)
    lane_at = lax.broadcasted_iota(jnp.int32, (block, block), 1)
    upper, lower, even = row_at < lane_at, row_at > lane_at, row_at == lane_at

    def gram_of(k):
        tile = data_ref[:, columns(k)]
        first, second = tile[:, :block], tile[:, block:]
        top = lax.dot_general(first, tile, (((0,), (0,)), ((), ())), preferred_element_type=F32)
        low = lax.dot_general(second, second, (((0,), (0,)), ((), ())), preferred_element_type=F32)
        gram[k, :, :block] = jnp.where(upper, top[:, :block], low).astype(BF16)
        gram[k, :, block:] = top[:, block:].astype(BF16)
        part1[k, 1:2, :block] = jnp.sum(jnp.where(even, top[:, :block], 0.0), axis=0, keepdims=True)
        part1[k, 1:2, block:] = jnp.sum(jnp.where(even, low, 0.0), axis=0, keepdims=True)
        left, right = first.astype(F32), second.astype(F32)
        return left * left + right * right

    def halving(source, target, index, sends, recvs, peer):
        return pltpu.make_async_remote_copy(
            src_ref=source, dst_ref=target.at[index], send_sem=sends.at[index],
            recv_sem=recvs.at[index], device_id=(peer,), device_id_type=MESH,
        )

    def copy_a(q, j):
        return halving(gram.at[8 * q + 2 * j + 1 - bit0], in_a, 4 * q + j, send_a, recv_a, partner)

    def order_of(q):
        swap = q % 2
        return (1 - swap) * bit1 + swap * bit2, 1 + swap, (1 - swap) * bit2 + swap * bit1, 2 - swap

    def copy_b(q, t):
        bit, weight, _, other = order_of(q)
        return halving(
            sum_a.at[4 * q + weight * (1 - bit) + other * t], in_b, 2 * q + t, send_b, recv_b,
            me + 2 * weight * (1 - 2 * bit),
        )

    def copy_c(q):
        _, _, bit, weight = order_of(q)
        return halving(sum_b.at[2 * q + 1 - bit], in_c, q, send_c, recv_c, me + 2 * weight * (1 - 2 * bit))

    def copy_d(q):
        return pltpu.make_async_remote_copy(
            src_ref=sum_c.at[q], dst_ref=gram_in.at[cube], send_sem=gram_send.at[0],
            recv_sem=gram_recv.at[0], device_id=(me + 8 * (q - cube),), device_id_type=MESH,
        )

    def added(x, y):
        return (x.astype(F32) + y.astype(F32)).astype(BF16)

    def turn(i):
        return jnp.where(i == cubes - 1, cube, far(jnp.minimum(i, cubes - 2)))

    def merge_a(i):
        q = turn(i)
        bit, weight, last, other = order_of(q)
        for t in (1 - last, last):
            for side in (1 - bit, bit):
                at = weight * side + other * t
                copy_a(q, at).wait_recv()
                sum_a[4 * q + at] = added(gram[8 * q + 2 * at + bit0], in_a[4 * q + at])
            copy_b(q, t).start()

    def merge_b(i):
        q = turn(i)
        bit, weight, last, other = order_of(q)
        for t in (1 - last, last):
            copy_b(q, t).wait_recv()
            sum_b[2 * q + t] = added(sum_a[4 * q + weight * bit + other * t], in_b[2 * q + t])
        copy_c(q).start()

    def merged_c(q):
        bit = order_of(q)[2]
        copy_c(q).wait_recv()
        return added(sum_b[2 * q + bit], in_c[q])

    def merge_c(i):
        q = turn(i)
        sum_c[q] = merged_c(q)
        copy_d(q).start()

    def gram_step(i, total):
        q = turn(i)
        for j in range(4):
            total = total + gram_of(8 * q + 2 * j + 1 - bit0)
            copy_a(q, j).start()
        for j in range(4):
            total = total + gram_of(8 * q + 2 * j + bit0)
        merge_a(i)
        return total

    half = cubes // 2
    square_total = lax.fori_loop(0, half, gram_step, jnp.zeros((feats, block), F32))
    total_wait(got0, 0).wait_recv()
    margin0 = jnp.sum(got0[...], axis=0)
    own0[...] = bound * sign * jnp.maximum(0.0, 1.0 - sign * margin0)
    gather_start(own0, all0, 0 + 3)

    def late_step(i, total):
        total = gram_step(i, total)
        merge_b(i - half)
        return total

    square_total = lax.fori_loop(half, cubes, late_step, square_total)
    column_sq = nt(jnp.ones((8, block), F32), square_total, HIGH)[0:1, :]
    ascent = back(all0, 3)
    loop(cubes - half, cubes, merge_b)
    loop(0, half, merge_c)
    scale = column_sq / samples + 1e-06
    stepped = w_start + ascent / (samples * scale)
    thresh = 1.0 / (4.0 * features * scale)
    primal = stepped - jnp.clip(stepped, -thresh, thresh)
    margin_scatter(primal, part1, got1, 1)
    loop(half, cubes - 1, merge_c)
    gram_in[cube] = merged_c(cube)

    orders, places = [], []
    for b in range(blocks):
        order = (lax.broadcasted_iota(jnp.int32, (block, block), 0) == visit_ref[b:b + 1, :]).astype(F32)
        orders.append(order)
        places.append(order.T.astype(BF16))

    alpha_zero = bound * frac_ref[...]

    def permute(vectors):
        stacked = jnp.concatenate(list(vectors) + [jnp.zeros((8 - len(vectors), rows), F32)], axis=0)
        return [nn(stacked[:, b * block:(b + 1) * block], orders[b], HIGH) for b in range(blocks)]

    total_wait(got1, 1).wait_recv()
    received = jnp.sum(got1[...], axis=0)
    margin1, diag = received[0:1, :], received[1:2, :]
    loss = jnp.sum(bound * jnp.square(jnp.maximum(0.0, 1.0 - sign * margin1)), axis=1, keepdims=True)
    penalty = jnp.sum(jnp.abs(primal), axis=1, keepdims=True)
    objective_part = loss / (2.0 * samples) + penalty / (4.0 * features)
    permuted = permute((sign, bound, alpha_zero, diag, margin1))
    sign_p = [x[0:1] for x in permuted]
    bound_p = [x[1:2] for x in permuted]
    zero_p = [x[2:3] for x in permuted]
    inverse_p = [0.5 / (x[3:4] + 1e-06) for x in permuted]
    margin_p = [x[4:5] for x in permuted]

    view = gram_in.at[pl.ds(0, cubes - 1)]
    gram_wait = pltpu.make_async_remote_copy(
        src_ref=view, dst_ref=view, send_sem=gram_send.at[0], recv_sem=gram_recv.at[0],
        device_id=(partner,), device_id_type=MESH,
    )
    gram_wait.wait_recv()
    full = jnp.sum(gram_in[...].astype(F32), axis=0)
    packed, cross = full[:, :block], full[:, block:]
    above, below = jnp.where(upper, packed, 0.0), jnp.where(lower, packed, 0.0)
    blocks_p = {}
    for (a, b), piece in {(0, 0): above + above.T, (0, 1): cross, (1, 1): below + below.T}.items():
        piece = nn(piece.astype(BF16), orders[b].astype(BF16)).astype(BF16)
        blocks_p[a, b] = nn(places[a], piece).astype(BF16)

    lane = lax.broadcasted_iota(jnp.int32, (1, block), 1)
    sub = lax.broadcasted_iota(jnp.int32, (ROWS, block), 0)

    def times_gram(delta, piece):
        high = delta.astype(BF16).astype(F32)
        lhs = jnp.where(sub == 0, high, jnp.where(sub == 1, delta - high, 0.0)).astype(BF16)
        return 2.0 * jnp.sum(nn(lhs, piece)[0:8], axis=0, keepdims=True)

    def sweep(alpha, margin):
        result, margin = [], list(margin)
        for b in range(blocks):
            now, m, moved = alpha[b], margin[b], jnp.zeros((1, block), F32)
            for s in range(block // GROUP):
                fresh = jnp.clip(now + (1.0 - sign_p[b] * m) * inverse_p[b], 0.0, bound_p[b])
                mine = (lane >= s * GROUP) & (lane < (s + 1) * GROUP)
                change = jnp.where(mine, fresh - now, 0.0)
                now = jnp.where(mine, fresh, now)
                change = sign_p[b] * change
                moved = moved + change
                if s + 1 < block // GROUP:
                    m = m + times_gram(change, blocks_p[b, b])
            for later in range(b + 1, blocks):
                margin[later] = margin[later] + times_gram(moved, blocks_p[b, later])
            result.append(now)
        return result

    def changes(after, before):
        pieces = []
        for b in range(blocks):
            z = spread(sign_p[b] * (after[b] - before[b]))
            pieces.append(nt(z, orders[b].astype(BF16))[0:1, :])
        return jnp.concatenate(pieces, axis=1)

    one_p = sweep(zero_p, margin_p)
    own1[0:1, 0:rows] = changes(one_p, zero_p)
    own1[0:1, rows:] = jnp.broadcast_to(objective_part, (1, block))
    gather_start(own1, all1, 1 + 3)
    update_one = back(all1, 4) * (2.0 / devices)
    margin_scatter(update_one, part2, got2, 2)
    out_ref[:, feats + rows:] = jnp.sum(all1[...], axis=0)[:, rows:]
    total_wait(got2, 2).wait_recv()
    margin2 = margin1 + jnp.sum(got2[...], axis=0)
    margin2_p = [x[0:1] for x in permute((margin2,))]
    two_p = sweep(one_p, margin2_p)
    own2[...] = changes(two_p, one_p)
    gather_start(own2, all2, 2 + 3)
    for b in range(blocks):
        spot = jnp.broadcast_to(two_p[b], (8, block))
        out_ref[:, feats + b * block:feats + (b + 1) * block] = nt(spot, orders[b], HIGH)[0:1, :]
    out_ref[:, :feats] = primal + update_one + back(all2, 5) * (2.0 / devices)

    for phase, ref in enumerate((got0, got1, got2)):
        total_wait(ref, phase).wait_send()
    for phase, ref in enumerate((all0, all1, all2)):
        total_wait(ref, phase + 3).wait_send()
    gram_wait.wait_send()

    def drain(q):
        for j in range(4):
            copy_a(q, j).wait_send()
        for j in range(2):
            copy_b(q, j).wait_send()
        copy_c(q).wait_send()

    loop(0, cubes, drain)


def body(devices, data_t, labels, sample_weight, w_start, alpha_start, visit_order):
    feats = data_t.shape[0]
    rows = alpha_start.shape[0]
    blocks, block = visit_order.shape
    cubes = devices // 8
    labels = labels.reshape(devices, 1, rows)
    bound = sample_weight.reshape(devices, 1, rows)

    def grams(count):
        return pltpu.VMEM((count, block, rows), BF16)

    def semaphores(count):
        return pltpu.SemaphoreType.DMA((count,))

    def vectors(height, length):
        return pltpu.VMEM((devices, height, length), F32)

    vmem = pl.BlockSpec(memory_space=pltpu.VMEM)
    out = pl.pallas_call(
        functools.partial(kernel, devices),
        name="svm_rounds",
        out_shape=jax.ShapeDtypeStruct((1, feats + rows + block), F32),
        in_specs=[pl.BlockSpec(memory_space=pl.ANY)] + [vmem] * 5,
        out_specs=vmem,
        scratch_shapes=[
            vectors(1, rows), vectors(2, rows), vectors(1, rows),
            vectors(1, rows), vectors(2, rows), vectors(1, rows),
            pltpu.VMEM((1, rows), F32), pltpu.VMEM((1, rows + block), F32), pltpu.VMEM((1, rows), F32),
            vectors(1, rows), vectors(1, rows + block), vectors(1, rows),
            pltpu.VMEM(data_t.shape, BF16), grams(devices), grams(4 * cubes), grams(2 * cubes), grams(cubes),
            grams(4 * cubes), grams(2 * cubes), grams(cubes), grams(cubes),
            semaphores(cubes), semaphores(6), semaphores(3), semaphores(3 * cubes), semaphores(4 * cubes), semaphores(4 * cubes),
            semaphores(2 * cubes), semaphores(2 * cubes), semaphores(cubes), semaphores(cubes),
            semaphores(1), semaphores(1),
        ],
        compiler_params=pltpu.CompilerParams(
            collective_id=0, has_side_effects=True, vmem_limit_bytes=63 * 1024 * 1024
        ),
    )(data_t, labels, bound, w_start[None], alpha_start[None], visit_order)
    return out[0, :feats], out[0, feats:feats + rows], out[0, feats + rows]


def solution(mesh):
    placed = (P("shard", None), P(), P(), P("shard"), P("shard"), P("shard", None))
    return jax.shard_map(
        functools.partial(body, mesh.shape["shard"]), mesh=mesh, in_specs=placed,
        out_specs=(P("shard"), P("shard"), P()), check_vma=False,
    )
```

```python
import functools

import jax
import jax.numpy as jnp
from jax import lax
from jax.experimental import pallas as pl
from jax.experimental.pallas import tpu as pltpu
from jax.sharding import PartitionSpec as P

GROUP = 16
ROWS = 16
MESH = pl.DeviceIdType.MESH
F32 = jnp.float32
BF16 = jnp.bfloat16
HIGH = lax.Precision.HIGHEST


def nn(a, b, precision=None):
    return lax.dot_general(a, b, (((1,), (0,)), ((), ())), preferred_element_type=F32, precision=precision)


def nt(a, b, precision=None):
    return lax.dot_general(a, b, (((1,), (1,)), ((), ())), preferred_element_type=F32, precision=precision)


def spread(row):
    return jnp.broadcast_to(row, (ROWS, row.shape[-1])).astype(BF16)


def kernel(
    devices, data_hbm, label_ref, bound_ref, start_ref, frac_ref, visit_ref,
    out_ref,
    part0, part1, part2, got0, got1, got2, own0, own1, own2, all0, all1, all2,
    data_ref, gram, in_a, in_b, in_c, sum_a, sum_b, sum_c, gram_in,
    load_sem, send_sem, recv_sem, gather_sem, send_a, recv_a, send_b, recv_b, send_c, recv_c, gram_send, gram_recv,
):
    me = lax.axis_index("shard")
    feats, samples = data_hbm.shape
    rows = label_ref.shape[2]
    blocks, block = visit_ref.shape
    features = feats * devices
    cubes = devices // 8
    cube = me // 8
    bit0, bit1, bit2 = me % 2, (me // 2) % 2, (me // 4) % 2
    partner = me + 1 - 2 * bit0

    def columns(k):
        return pl.ds(pl.multiple_of(k * rows, rows), rows)

    def loop(first, last, action):
        def step(i, carry):
            action(i)
            return carry

        lax.fori_loop(first, last, step, 0)

    upward = cube // (cubes // 2)

    def near(i):
        place = upward * (cubes - 2 - i) + (1 - upward) * i
        return place + jnp.where(place >= cube, 1, 0)

    def far(i):
        return near(cubes - 2 - i)

    def mates(action):
        loop(1, 8, lambda i: action(8 * cube + lax.rem(me + i, 8)))

    def cube_of(q, action):
        loop(0, 8, lambda j: action(8 * q + j))

    def peers(action):
        loop(0, cubes - 1, lambda i: cube_of(far(i), action))
        mates(action)

    def remote(source, target, send, recv, peer):
        return pltpu.make_async_remote_copy(
            src_ref=source, dst_ref=target, send_sem=send, recv_sem=recv,
            device_id=(peer,), device_id_type=MESH,
        )

    def total_wait(ref, phase):
        view = ref.at[pl.ds(0, devices - 1)]
        return remote(view, view, send_sem.at[phase], recv_sem.at[phase % 3], partner)

    def scatter_send(part, got, phase):
        def send(peer):
            remote(part.at[peer], got.at[me], send_sem.at[phase], recv_sem.at[phase], peer).start()

        return send

    def gather_start(own, everyone, phase):
        everyone[me] = own[...]
        spot = (phase - 3) * cubes + cube
        peers(lambda peer: remote(own, everyone.at[me], send_sem.at[phase], gather_sem.at[spot], peer).start())

    def part_of(lhs, part, q):
        for j in range(8):
            k = 8 * q + j
            part[k, 0:1, :] = nn(lhs, data_ref[:, columns(k)])[0:1, :]

    def margin_scatter(row, part, got, phase):
        lhs = spread(row)
        send = scatter_send(part, got, phase)

        def step(i):
            q = far(i)
            part_of(lhs, part, q)
            cube_of(q, send)

        loop(0, cubes - 1, step)
        part_of(lhs, part, cube)
        mates(send)
        got[me] = part[me]

    def back(everyone, phase):
        def arrival(q, count):
            view = everyone.at[pl.ds(8 * q, count)]
            spot = (phase - 3) * cubes + q
            remote(view, view, send_sem.at[phase], gather_sem.at[spot], partner).wait_recv()

        def cube_sum(q, total):
            for j in range(8):
                k = 8 * q + j
                total = total + nt(spread(everyone[k][0:1, 0:rows]), data_ref[:, columns(k)])
            return total

        def step(i, total):
            q = near(i)
            arrival(q, 8)
            return cube_sum(q, total)

        arrival(cube, 7)
        total = cube_sum(cube, jnp.zeros((ROWS, feats), F32))
        return lax.fori_loop(0, cubes - 1, step, total)[0:1, :]

    def load(q):
        view = pl.ds(pl.multiple_of(8 * q * rows, rows), 8 * rows)
        return pltpu.make_async_copy(data_hbm.at[:, view], data_ref.at[:, view], load_sem.at[q])

    loop(0, cubes - 1, lambda i: load(far(i)).start())
    load(cube).start()
    barrier = pltpu.get_barrier_semaphore()
    peers(lambda peer: pl.semaphore_signal(barrier, inc=1, device_id=(peer,), device_id_type=MESH))

    w_start = start_ref[...]
    sign, bound = label_ref[me].astype(F32), bound_ref[me]
    start_rows = spread(w_start)

    def first_part(q):
        load(q).wait()
        part_of(start_rows, part0, q)

    loop(0, cubes - 1, lambda i: first_part(far(i)))
    first_part(cube)
    pl.semaphore_wait(barrier, devices - 1)
    peers(scatter_send(part0, got0, 0))
    got0[me] = part0[me]

    row_at = lax.broadcasted_iota(jnp.int32, (block, block), 0)
    lane_at = lax.broadcasted_iota(jnp.int32, (block, block), 1)
    upper, lower, even = row_at < lane_at, row_at > lane_at, row_at == lane_at

    def gram_of(k):
        tile = data_ref[:, columns(k)]
        first, second = tile[:, :block], tile[:, block:]
        top = lax.dot_general(first, tile, (((0,), (0,)), ((), ())), preferred_element_type=F32)
        low = lax.dot_general(second, second, (((0,), (0,)), ((), ())), preferred_element_type=F32)
        gram[k, :, :block] = jnp.where(upper, top[:, :block], low).astype(BF16)
        gram[k, :, block:] = top[:, block:].astype(BF16)
        part1[k, 1:2, :block] = jnp.sum(jnp.where(even, top[:, :block], 0.0), axis=0, keepdims=True)
        part1[k, 1:2, block:] = jnp.sum(jnp.where(even, low, 0.0), axis=0, keepdims=True)
        left, right = first.astype(F32), second.astype(F32)
        return left * left + right * right

    def halving(source, target, index, sends, recvs, peer):
        return pltpu.make_async_remote_copy(
            src_ref=source, dst_ref=target.at[index], send_sem=sends.at[index],
            recv_sem=recvs.at[index], device_id=(peer,), device_id_type=MESH,
        )

    def copy_a(q, j):
        return halving(gram.at[8 * q + 2 * j + 1 - bit0], in_a, 4 * q + j, send_a, recv_a, partner)

    def order_of(q):
        swap = q % 2
        return (1 - swap) * bit1 + swap * bit2, 1 + swap, (1 - swap) * bit2 + swap * bit1, 2 - swap

    def copy_b(q, t):
        bit, weight, _, other = order_of(q)
        return halving(
            sum_a.at[4 * q + weight * (1 - bit) + other * t], in_b, 2 * q + t, send_b, recv_b,
            me + 2 * weight * (1 - 2 * bit),
        )

    def copy_c(q):
        _, _, bit, weight = order_of(q)
        return halving(sum_b.at[2 * q + 1 - bit], in_c, q, send_c, recv_c, me + 2 * weight * (1 - 2 * bit))

    def copy_d(q):
        return pltpu.make_async_remote_copy(
            src_ref=sum_c.at[q], dst_ref=gram_in.at[cube], send_sem=gram_send.at[0],
            recv_sem=gram_recv.at[0], device_id=(me + 8 * (q - cube),), device_id_type=MESH,
        )

    def added(x, y):
        return (x.astype(F32) + y.astype(F32)).astype(BF16)

    def turn(i):
        return jnp.where(i == cubes - 1, cube, far(jnp.minimum(i, cubes - 2)))

    def merge_a(i):
        q = turn(i)
        bit, weight, last, other = order_of(q)
        for t in (1 - last, last):
            for side in (1 - bit, bit):
                at = weight * side + other * t
                copy_a(q, at).wait_recv()
                sum_a[4 * q + at] = added(gram[8 * q + 2 * at + bit0], in_a[4 * q + at])
            copy_b(q, t).start()

    def merge_b(i):
        q = turn(i)
        bit, weight, last, other = order_of(q)
        for t in (1 - last, last):
            copy_b(q, t).wait_recv()
            sum_b[2 * q + t] = added(sum_a[4 * q + weight * bit + other * t], in_b[2 * q + t])
        copy_c(q).start()

    def merged_c(q):
        bit = order_of(q)[2]
        copy_c(q).wait_recv()
        return added(sum_b[2 * q + bit], in_c[q])

    def merge_c(i):
        q = turn(i)
        sum_c[q] = merged_c(q)
        copy_d(q).start()

    def gram_step(i, total):
        q = turn(i)
        for j in range(4):
            total = total + gram_of(8 * q + 2 * j + 1 - bit0)
        for j in range(4):
            copy_a(q, j).start()
        for j in range(4):
            total = total + gram_of(8 * q + 2 * j + bit0)
        merge_a(i)
        return total

    half = cubes // 2
    square_total = lax.fori_loop(0, half, gram_step, jnp.zeros((feats, block), F32))
    total_wait(got0, 0).wait_recv()
    margin0 = jnp.sum(got0[...], axis=0)
    own0[...] = bound * sign * jnp.maximum(0.0, 1.0 - sign * margin0)
    gather_start(own0, all0, 0 + 3)

    def late_step(i, total):
        total = gram_step(i, total)
        merge_b(i - half)
        return total

    square_total = lax.fori_loop(half, cubes, late_step, square_total)
    column_sq = nt(jnp.ones((8, block), F32), square_total, HIGH)[0:1, :]
    ascent = back(all0, 3)
    loop(cubes - half, cubes - 1, merge_b)
    scale = column_sq / samples + 1e-06
    stepped = w_start + ascent / (samples * scale)
    thresh = 1.0 / (4.0 * features * scale)
    primal = stepped - jnp.clip(stepped, -thresh, thresh)
    margin_scatter(primal, part1, got1, 1)
    merge_b(cubes - 1)
    loop(0, cubes - 1, merge_c)
    gram_in[cube] = merged_c(cube)

    orders, places = [], []
    for b in range(blocks):
        order = (lax.broadcasted_iota(jnp.int32, (block, block), 0) == visit_ref[b:b + 1, :]).astype(F32)
        orders.append(order)
        places.append(order.T.astype(BF16))

    alpha_zero = bound * frac_ref[...]

    def permute(vectors):
        stacked = jnp.concatenate(list(vectors) + [jnp.zeros((8 - len(vectors), rows), F32)], axis=0)
        return [nn(stacked[:, b * block:(b + 1) * block], orders[b], HIGH) for b in range(blocks)]

    total_wait(got1, 1).wait_recv()
    received = jnp.sum(got1[...], axis=0)
    margin1, diag = received[0:1, :], received[1:2, :]
    loss = jnp.sum(bound * jnp.square(jnp.maximum(0.0, 1.0 - sign * margin1)), axis=1, keepdims=True)
    penalty = jnp.sum(jnp.abs(primal), axis=1, keepdims=True)
    objective_part = loss / (2.0 * samples) + penalty / (4.0 * features)
    permuted = permute((sign, bound, alpha_zero, diag, margin1))
    sign_p = [x[0:1] for x in permuted]
    bound_p = [x[1:2] for x in permuted]
    zero_p = [x[2:3] for x in permuted]
    inverse_p = [0.5 / (x[3:4] + 1e-06) for x in permuted]
    margin_p = [x[4:5] for x in permuted]

    view = gram_in.at[pl.ds(0, cubes - 1)]
    gram_wait = pltpu.make_async_remote_copy(
        src_ref=view, dst_ref=view, send_sem=gram_send.at[0], recv_sem=gram_recv.at[0],
        device_id=(partner,), device_id_type=MESH,
    )
    gram_wait.wait_recv()
    full = jnp.sum(gram_in[...].astype(F32), axis=0)
    packed, cross = full[:, :block], full[:, block:]
    above, below = jnp.where(upper, packed, 0.0), jnp.where(lower, packed, 0.0)
    blocks_p = {}
    for (a, b), piece in {(0, 0): above + above.T, (0, 1): cross, (1, 1): below + below.T}.items():
        piece = nn(piece.astype(BF16), orders[b].astype(BF16)).astype(BF16)
        blocks_p[a, b] = nn(places[a], piece).astype(BF16)

    lane = lax.broadcasted_iota(jnp.int32, (1, block), 1)
    sub = lax.broadcasted_iota(jnp.int32, (ROWS, block), 0)

    def times_gram(delta, piece):
        high = delta.astype(BF16).astype(F32)
        lhs = jnp.where(sub == 0, high, jnp.where(sub == 1, delta - high, 0.0)).astype(BF16)
        return 2.0 * jnp.sum(nn(lhs, piece)[0:8], axis=0, keepdims=True)

    def sweep(alpha, margin):
        result, margin = [], list(margin)
        for b in range(blocks):
            now, m, moved = alpha[b], margin[b], jnp.zeros((1, block), F32)
            for s in range(block // GROUP):
                fresh = jnp.clip(now + (1.0 - sign_p[b] * m) * inverse_p[b], 0.0, bound_p[b])
                mine = (lane >= s * GROUP) & (lane < (s + 1) * GROUP)
                change = jnp.where(mine, fresh - now, 0.0)
                now = jnp.where(mine, fresh, now)
                change = sign_p[b] * change
                moved = moved + change
                if s + 1 < block // GROUP:
                    m = m + times_gram(change, blocks_p[b, b])
            for later in range(b + 1, blocks):
                margin[later] = margin[later] + times_gram(moved, blocks_p[b, later])
            result.append(now)
        return result

    def changes(after, before):
        pieces = []
        for b in range(blocks):
            z = spread(sign_p[b] * (after[b] - before[b]))
            pieces.append(nt(z, orders[b].astype(BF16))[0:1, :])
        return jnp.concatenate(pieces, axis=1)

    one_p = sweep(zero_p, margin_p)
    own1[0:1, 0:rows] = changes(one_p, zero_p)
    own1[0:1, rows:] = jnp.broadcast_to(objective_part, (1, block))
    gather_start(own1, all1, 1 + 3)
    update_one = back(all1, 4) * (2.0 / devices)
    margin_scatter(update_one, part2, got2, 2)
    out_ref[:, feats + rows:] = jnp.sum(all1[...], axis=0)[:, rows:]
    total_wait(got2, 2).wait_recv()
    margin2 = margin1 + jnp.sum(got2[...], axis=0)
    margin2_p = [x[0:1] for x in permute((margin2,))]
    two_p = sweep(one_p, margin2_p)
    own2[...] = changes(two_p, one_p)
    gather_start(own2, all2, 2 + 3)
    for b in range(blocks):
        spot = jnp.broadcast_to(two_p[b], (8, block))
        out_ref[:, feats + b * block:feats + (b + 1) * block] = nt(spot, orders[b], HIGH)[0:1, :]
    out_ref[:, :feats] = primal + update_one + back(all2, 5) * (2.0 / devices)

    for phase, ref in enumerate((got0, got1, got2)):
        total_wait(ref, phase).wait_send()
    for phase, ref in enumerate((all0, all1, all2)):
        total_wait(ref, phase + 3).wait_send()
    gram_wait.wait_send()

    def drain(q):
        for j in range(4):
            copy_a(q, j).wait_send()
        for j in range(2):
            copy_b(q, j).wait_send()
        copy_c(q).wait_send()

    loop(0, cubes, drain)


def body(devices, data_t, labels, sample_weight, w_start, alpha_start, visit_order):
    feats = data_t.shape[0]
    rows = alpha_start.shape[0]
    blocks, block = visit_order.shape
    cubes = devices // 8
    labels = labels.reshape(devices, 1, rows)
    bound = sample_weight.reshape(devices, 1, rows)

    def grams(count):
        return pltpu.VMEM((count, block, rows), BF16)

    def semaphores(count):
        return pltpu.SemaphoreType.DMA((count,))

    def vectors(height, length):
        return pltpu.VMEM((devices, height, length), F32)

    vmem = pl.BlockSpec(memory_space=pltpu.VMEM)
    out = pl.pallas_call(
        functools.partial(kernel, devices),
        name="svm_rounds",
        out_shape=jax.ShapeDtypeStruct((1, feats + rows + block), F32),
        in_specs=[pl.BlockSpec(memory_space=pl.ANY)] + [vmem] * 5,
        out_specs=vmem,
        scratch_shapes=[
            vectors(1, rows), vectors(2, rows), vectors(1, rows),
            vectors(1, rows), vectors(2, rows), vectors(1, rows),
            pltpu.VMEM((1, rows), F32), pltpu.VMEM((1, rows + block), F32), pltpu.VMEM((1, rows), F32),
            vectors(1, rows), vectors(1, rows + block), vectors(1, rows),
            pltpu.VMEM(data_t.shape, BF16), grams(devices), grams(4 * cubes), grams(2 * cubes), grams(cubes),
            grams(4 * cubes), grams(2 * cubes), grams(cubes), grams(cubes),
            semaphores(cubes), semaphores(6), semaphores(3), semaphores(3 * cubes), semaphores(4 * cubes), semaphores(4 * cubes),
            semaphores(2 * cubes), semaphores(2 * cubes), semaphores(cubes), semaphores(cubes),
            semaphores(1), semaphores(1),
        ],
        compiler_params=pltpu.CompilerParams(
            collective_id=0, has_side_effects=True, vmem_limit_bytes=63 * 1024 * 1024
        ),
    )(data_t, labels, bound, w_start[None], alpha_start[None], visit_order)
    return out[0, :feats], out[0, feats:feats + rows], out[0, feats + rows]


def solution(mesh):
    placed = (P("shard", None), P(), P(), P("shard"), P("shard"), P("shard", None))
    return jax.shard_map(
        functools.partial(body, mesh.shape["shard"]), mesh=mesh, in_specs=placed,
        out_specs=(P("shard"), P("shard"), P()), check_vma=False,
    )
```

```python
import functools

import jax
import jax.numpy as jnp
from jax import lax
from jax.experimental import pallas as pl
from jax.experimental.pallas import tpu as pltpu
from jax.sharding import PartitionSpec as P

GROUP = 16
ROWS = 16
MESH = pl.DeviceIdType.MESH
F32 = jnp.float32
BF16 = jnp.bfloat16
HIGH = lax.Precision.HIGHEST


def nn(a, b, precision=None):
    return lax.dot_general(a, b, (((1,), (0,)), ((), ())), preferred_element_type=F32, precision=precision)


def nt(a, b, precision=None):
    return lax.dot_general(a, b, (((1,), (1,)), ((), ())), preferred_element_type=F32, precision=precision)


def spread(row):
    return jnp.broadcast_to(row, (ROWS, row.shape[-1])).astype(BF16)


def kernel(
    devices, data_hbm, label_ref, bound_ref, start_ref, frac_ref, visit_ref,
    out_ref, objective_ref,
    part0, part1, part2, got0, got1, got2, own0, own1, own2, all0, all1, all2,
    data_ref, gram, in_a, in_b, in_c, sum_a, sum_b, sum_c, gram_in,
    load_sem, send_sem, recv_sem, gather_sem, send_a, recv_a, send_b, recv_b, send_c, recv_c, gram_send, gram_recv,
):
    me = lax.axis_index("shard")
    feats, samples = data_hbm.shape
    rows = label_ref.shape[2]
    blocks, block = visit_ref.shape
    features = feats * devices
    cubes = devices // 8
    cube = me // 8
    bit0, bit1, bit2 = me % 2, (me // 2) % 2, (me // 4) % 2
    partner = me + 1 - 2 * bit0

    def columns(k):
        return pl.ds(pl.multiple_of(k * rows, rows), rows)

    def loop(first, last, action):
        def step(i, carry):
            action(i)
            return carry

        lax.fori_loop(first, last, step, 0)

    upward = cube // (cubes // 2)

    def near(i):
        place = upward * (cubes - 2 - i) + (1 - upward) * i
        return place + jnp.where(place >= cube, 1, 0)

    def far(i):
        return near(cubes - 2 - i)

    def mates(action):
        loop(1, 8, lambda i: action(8 * cube + lax.rem(me + i, 8)))

    def cube_of(q, action):
        loop(0, 8, lambda j: action(8 * q + j))

    def peers(action):
        loop(0, cubes - 1, lambda i: cube_of(far(i), action))
        mates(action)

    def remote(source, target, send, recv, peer):
        return pltpu.make_async_remote_copy(
            src_ref=source, dst_ref=target, send_sem=send, recv_sem=recv,
            device_id=(peer,), device_id_type=MESH,
        )

    def total_wait(ref, phase):
        view = ref.at[pl.ds(0, devices - 1)]
        return remote(view, view, send_sem.at[phase], recv_sem.at[phase % 3], partner)

    def scatter_send(part, got, phase):
        def send(peer):
            remote(part.at[peer], got.at[me], send_sem.at[phase], recv_sem.at[phase], peer).start()

        return send

    def gather_start(own, everyone, phase):
        everyone[me] = own[...]
        spot = (phase - 3) * cubes + cube
        peers(lambda peer: remote(own, everyone.at[me], send_sem.at[phase], gather_sem.at[spot], peer).start())

    def part_of(lhs, part, q):
        for j in range(8):
            k = 8 * q + j
            part[k, 0:1, :] = nn(lhs, data_ref[:, columns(k)])[0:1, :]

    def margin_scatter(row, part, got, phase):
        lhs = spread(row)
        send = scatter_send(part, got, phase)

        def step(i):
            q = far(i)
            part_of(lhs, part, q)
            cube_of(q, send)

        loop(0, cubes - 1, step)
        part_of(lhs, part, cube)
        mates(send)
        got[me] = part[me]

    def back(everyone, phase):
        def arrival(q, count):
            view = everyone.at[pl.ds(8 * q, count)]
            spot = (phase - 3) * cubes + q
            remote(view, view, send_sem.at[phase], gather_sem.at[spot], partner).wait_recv()

        def cube_sum(q, total):
            for j in range(8):
                k = 8 * q + j
                total = total + nt(spread(everyone[k][0:1, 0:rows]), data_ref[:, columns(k)])
            return total

        def step(i, total):
            q = near(i)
            arrival(q, 8)
            return cube_sum(q, total)

        arrival(cube, 7)
        total = cube_sum(cube, jnp.zeros((ROWS, feats), F32))
        return lax.fori_loop(0, cubes - 1, step, total)[0:1, :]

    def load(q):
        view = pl.ds(pl.multiple_of(8 * q * rows, rows), 8 * rows)
        return pltpu.make_async_copy(data_hbm.at[:, view], data_ref.at[:, view], load_sem.at[q])

    loop(0, cubes - 1, lambda i: load(far(i)).start())
    load(cube).start()
    barrier = pltpu.get_barrier_semaphore()
    peers(lambda peer: pl.semaphore_signal(barrier, inc=1, device_id=(peer,), device_id_type=MESH))

    w_start = start_ref[...]
    sign, bound = label_ref[me].astype(F32), bound_ref[me]
    start_rows = spread(w_start)

    def first_part(q):
        load(q).wait()
        part_of(start_rows, part0, q)

    loop(0, cubes - 1, lambda i: first_part(far(i)))
    first_part(cube)
    pl.semaphore_wait(barrier, devices - 1)
    peers(scatter_send(part0, got0, 0))
    got0[me] = part0[me]

    row_at = lax.broadcasted_iota(jnp.int32, (block, block), 0)
    lane_at = lax.broadcasted_iota(jnp.int32, (block, block), 1)
    upper, lower, even = row_at < lane_at, row_at > lane_at, row_at == lane_at

    def gram_of(k):
        tile = data_ref[:, columns(k)]
        first, second = tile[:, :block], tile[:, block:]
        top = lax.dot_general(first, tile, (((0,), (0,)), ((), ())), preferred_element_type=F32)
        low = lax.dot_general(second, second, (((0,), (0,)), ((), ())), preferred_element_type=F32)
        gram[k, :, :block] = jnp.where(upper, top[:, :block], low).astype(BF16)
        gram[k, :, block:] = top[:, block:].astype(BF16)
        part1[k, 1:2, :block] = jnp.sum(jnp.where(even, top[:, :block], 0.0), axis=0, keepdims=True)
        part1[k, 1:2, block:] = jnp.sum(jnp.where(even, low, 0.0), axis=0, keepdims=True)
        left, right = first.astype(F32), second.astype(F32)
        return left * left + right * right

    def halving(source, target, index, sends, recvs, peer):
        return pltpu.make_async_remote_copy(
            src_ref=source, dst_ref=target.at[index], send_sem=sends.at[index],
            recv_sem=recvs.at[index], device_id=(peer,), device_id_type=MESH,
        )

    def copy_a(q, j):
        return halving(gram.at[8 * q + 2 * j + 1 - bit0], in_a, 4 * q + j, send_a, recv_a, partner)

    def order_of(q):
        swap = q % 2
        return (1 - swap) * bit1 + swap * bit2, 1 + swap, (1 - swap) * bit2 + swap * bit1, 2 - swap

    def copy_b(q, t):
        bit, weight, _, other = order_of(q)
        return halving(
            sum_a.at[4 * q + weight * (1 - bit) + other * t], in_b, 2 * q + t, send_b, recv_b,
            me + 2 * weight * (1 - 2 * bit),
        )

    def copy_c(q):
        _, _, bit, weight = order_of(q)
        return halving(sum_b.at[2 * q + 1 - bit], in_c, q, send_c, recv_c, me + 2 * weight * (1 - 2 * bit))

    def copy_d(q):
        return pltpu.make_async_remote_copy(
            src_ref=sum_c.at[q], dst_ref=gram_in.at[cube], send_sem=gram_send.at[0],
            recv_sem=gram_recv.at[0], device_id=(me + 8 * (q - cube),), device_id_type=MESH,
        )

    def added(x, y):
        return (x.astype(F32) + y.astype(F32)).astype(BF16)

    def turn(i):
        return jnp.where(i == cubes - 1, cube, far(jnp.minimum(i, cubes - 2)))

    def merge_a(i):
        q = turn(i)
        bit, weight, last, other = order_of(q)
        for t in (1 - last, last):
            for side in (1 - bit, bit):
                at = weight * side + other * t
                copy_a(q, at).wait_recv()
                sum_a[4 * q + at] = added(gram[8 * q + 2 * at + bit0], in_a[4 * q + at])
            copy_b(q, t).start()

    def merge_b(i):
        q = turn(i)
        bit, weight, last, other = order_of(q)
        for t in (1 - last, last):
            copy_b(q, t).wait_recv()
            sum_b[2 * q + t] = added(sum_a[4 * q + weight * bit + other * t], in_b[2 * q + t])
        copy_c(q).start()

    def merged_c(q):
        bit = order_of(q)[2]
        copy_c(q).wait_recv()
        return added(sum_b[2 * q + bit], in_c[q])

    def merge_c(i):
        q = turn(i)
        sum_c[q] = merged_c(q)
        copy_d(q).start()

    def gram_step(i, total):
        q = turn(i)
        for j in range(4):
            total = total + gram_of(8 * q + 2 * j + 1 - bit0)
        for j in range(4):
            copy_a(q, j).start()
        for j in range(4):
            total = total + gram_of(8 * q + 2 * j + bit0)
        merge_a(i)
        return total

    half = cubes // 2
    square_total = lax.fori_loop(0, half, gram_step, jnp.zeros((feats, block), F32))
    total_wait(got0, 0).wait_recv()
    margin0 = jnp.sum(got0[...], axis=0)
    own0[...] = bound * sign * jnp.maximum(0.0, 1.0 - sign * margin0)
    gather_start(own0, all0, 0 + 3)

    def late_step(i, total):
        total = gram_step(i, total)
        merge_b(i - half)
        return total

    square_total = lax.fori_loop(half, cubes, late_step, square_total)
    column_sq = nt(jnp.ones((8, block), F32), square_total, HIGH)[0:1, :]
    ascent = back(all0, 3)
    loop(cubes - half, cubes - 1, merge_b)
    loop(0, half - 1, merge_c)
    scale = column_sq / samples + 1e-06
    stepped = w_start + ascent / (samples * scale)
    thresh = 1.0 / (4.0 * features * scale)
    primal = stepped - jnp.clip(stepped, -thresh, thresh)
    margin_scatter(primal, part1, got1, 1)
    loop(half - 1, half, merge_c)
    merge_b(cubes - 1)
    loop(half, cubes - 1, merge_c)
    gram_in[cube] = merged_c(cube)

    orders, places = [], []
    for b in range(blocks):
        order = (lax.broadcasted_iota(jnp.int32, (block, block), 0) == visit_ref[b:b + 1, :]).astype(F32)
        orders.append(order)
        places.append(order.T.astype(BF16))

    alpha_zero = bound * frac_ref[...]

    def permute(vectors):
        stacked = jnp.concatenate(list(vectors) + [jnp.zeros((8 - len(vectors), rows), F32)], axis=0)
        return [nn(stacked[:, b * block:(b + 1) * block], orders[b], HIGH) for b in range(blocks)]

    total_wait(got1, 1).wait_recv()
    received = jnp.sum(got1[...], axis=0)
    margin1, diag = received[0:1, :], received[1:2, :]
    loss = jnp.sum(bound * jnp.square(jnp.maximum(0.0, 1.0 - sign * margin1)), axis=1, keepdims=True)
    penalty = jnp.sum(jnp.abs(primal), axis=1, keepdims=True)
    objective_part = loss / (2.0 * samples) + penalty / (4.0 * features)
    permuted = permute((sign, bound, alpha_zero, diag, margin1))
    sign_p = [x[0:1] for x in permuted]
    bound_p = [x[1:2] for x in permuted]
    zero_p = [x[2:3] for x in permuted]
    inverse_p = [0.5 / (x[3:4] + 1e-06) for x in permuted]
    margin_p = [x[4:5] for x in permuted]

    view = gram_in.at[pl.ds(0, cubes - 1)]
    gram_wait = pltpu.make_async_remote_copy(
        src_ref=view, dst_ref=view, send_sem=gram_send.at[0], recv_sem=gram_recv.at[0],
        device_id=(partner,), device_id_type=MESH,
    )
    gram_wait.wait_recv()
    full = jnp.sum(gram_in[...].astype(F32), axis=0)
    packed, cross = full[:, :block], full[:, block:]
    above, below = jnp.where(upper, packed, 0.0), jnp.where(lower, packed, 0.0)
    blocks_p = {}
    for (a, b), piece in {(0, 0): above + above.T, (0, 1): cross, (1, 1): below + below.T}.items():
        piece = nn(piece.astype(BF16), orders[b].astype(BF16)).astype(BF16)
        blocks_p[a, b] = nn(places[a], piece).astype(BF16)

    lane = lax.broadcasted_iota(jnp.int32, (1, block), 1)
    sub = lax.broadcasted_iota(jnp.int32, (ROWS, block), 0)

    def times_gram(delta, piece):
        high = delta.astype(BF16).astype(F32)
        lhs = jnp.where(sub == 0, high, jnp.where(sub == 1, delta - high, 0.0)).astype(BF16)
        return 2.0 * jnp.sum(nn(lhs, piece)[0:8], axis=0, keepdims=True)

    def sweep(alpha, margin):
        result, margin = [], list(margin)
        for b in range(blocks):
            now, m, moved = alpha[b], margin[b], jnp.zeros((1, block), F32)
            for s in range(block // GROUP):
                fresh = jnp.clip(now + (1.0 - sign_p[b] * m) * inverse_p[b], 0.0, bound_p[b])
                mine = (lane >= s * GROUP) & (lane < (s + 1) * GROUP)
                change = jnp.where(mine, fresh - now, 0.0)
                now = jnp.where(mine, fresh, now)
                change = sign_p[b] * change
                moved = moved + change
                if s + 1 < block // GROUP:
                    m = m + times_gram(change, blocks_p[b, b])
            for later in range(b + 1, blocks):
                margin[later] = margin[later] + times_gram(moved, blocks_p[b, later])
            result.append(now)
        return result

    def changes(after, before):
        pieces = []
        for b in range(blocks):
            z = spread(sign_p[b] * (after[b] - before[b]))
            pieces.append(nt(z, orders[b].astype(BF16))[0:1, :])
        return jnp.concatenate(pieces, axis=1)

    one_p = sweep(zero_p, margin_p)
    own1[0:1, 0:rows] = changes(one_p, zero_p)
    own1[0:1, rows:] = jnp.broadcast_to(objective_part, (1, block))
    gather_start(own1, all1, 1 + 3)
    update_one = back(all1, 4) * (2.0 / devices)
    margin_scatter(update_one, part2, got2, 2)
    objective_ref[...] = jnp.sum(all1[...], axis=0)[:, rows:]
    total_wait(got2, 2).wait_recv()
    margin2 = margin1 + jnp.sum(got2[...], axis=0)
    margin2_p = [x[0:1] for x in permute((margin2,))]
    two_p = sweep(one_p, margin2_p)
    own2[...] = changes(two_p, one_p)
    gather_start(own2, all2, 2 + 3)
    for b in range(blocks):
        spot = jnp.broadcast_to(two_p[b], (8, block))
        out_ref[:, feats + b * block:feats + (b + 1) * block] = nt(spot, orders[b], HIGH)[0:1, :]
    out_ref[:, :feats] = primal + update_one + back(all2, 5) * (2.0 / devices)

    for phase, ref in enumerate((got0, got1, got2)):
        total_wait(ref, phase).wait_send()
    for phase, ref in enumerate((all0, all1, all2)):
        total_wait(ref, phase + 3).wait_send()
    gram_wait.wait_send()

    def drain(q):
        for j in range(4):
            copy_a(q, j).wait_send()
        for j in range(2):
            copy_b(q, j).wait_send()
        copy_c(q).wait_send()

    loop(0, cubes, drain)


def body(devices, data_t, labels, sample_weight, w_start, alpha_start, visit_order):
    feats = data_t.shape[0]
    rows = alpha_start.shape[0]
    blocks, block = visit_order.shape
    cubes = devices // 8
    labels = labels.reshape(devices, 1, rows)
    bound = sample_weight.reshape(devices, 1, rows)

    def grams(count):
        return pltpu.VMEM((count, block, rows), BF16)

    def semaphores(count):
        return pltpu.SemaphoreType.DMA((count,))

    def vectors(height, length):
        return pltpu.VMEM((devices, height, length), F32)

    vmem = pl.BlockSpec(memory_space=pltpu.VMEM)
    out, objective = pl.pallas_call(
        functools.partial(kernel, devices),
        name="svm_rounds",
        out_shape=(
            jax.ShapeDtypeStruct((1, feats + rows), F32),
            jax.ShapeDtypeStruct((1, block), F32),
        ),
        in_specs=[pl.BlockSpec(memory_space=pl.ANY)] + [vmem] * 5,
        out_specs=(vmem, vmem),
        scratch_shapes=[
            vectors(1, rows), vectors(2, rows), vectors(1, rows),
            vectors(1, rows), vectors(2, rows), vectors(1, rows),
            pltpu.VMEM((1, rows), F32), pltpu.VMEM((1, rows + block), F32), pltpu.VMEM((1, rows), F32),
            vectors(1, rows), vectors(1, rows + block), vectors(1, rows),
            pltpu.VMEM(data_t.shape, BF16), grams(devices), grams(4 * cubes), grams(2 * cubes), grams(cubes),
            grams(4 * cubes), grams(2 * cubes), grams(cubes), grams(cubes),
            semaphores(cubes), semaphores(6), semaphores(3), semaphores(3 * cubes), semaphores(4 * cubes), semaphores(4 * cubes),
            semaphores(2 * cubes), semaphores(2 * cubes), semaphores(cubes), semaphores(cubes),
            semaphores(1), semaphores(1),
        ],
        compiler_params=pltpu.CompilerParams(
            collective_id=0, has_side_effects=True, vmem_limit_bytes=63 * 1024 * 1024
        ),
    )(data_t, labels, bound, w_start[None], alpha_start[None], visit_order)
    return out[0, :feats], out[0, feats:feats + rows], objective[0, 0]


def solution(mesh):
    placed = (P("shard", None), P(), P(), P("shard"), P("shard"), P("shard", None))
    return jax.shard_map(
        functools.partial(body, mesh.shape["shard"]), mesh=mesh, in_specs=placed,
        out_specs=(P("shard"), P("shard"), P()), check_vma=False,
    )
```

```python
import functools

import jax
import jax.numpy as jnp
from jax import lax
from jax.experimental import pallas as pl
from jax.experimental.pallas import tpu as pltpu
from jax.sharding import PartitionSpec as P

GROUP = 16
ROWS = 16
MESH = pl.DeviceIdType.MESH
F32 = jnp.float32
BF16 = jnp.bfloat16
HIGH = lax.Precision.HIGHEST


def nn(a, b, precision=None):
    return lax.dot_general(a, b, (((1,), (0,)), ((), ())), preferred_element_type=F32, precision=precision)


def nt(a, b, precision=None):
    return lax.dot_general(a, b, (((1,), (1,)), ((), ())), preferred_element_type=F32, precision=precision)


def spread(row):
    return jnp.broadcast_to(row, (ROWS, row.shape[-1])).astype(BF16)


def kernel(
    devices, data_hbm, label_ref, bound_ref, start_ref, frac_ref, visit_ref,
    out_ref, objective_ref,
    part0, part1, part2, got0, got1, got2, own0, own1, own2, all0, all1, all2,
    data_ref, gram, in_a, in_b, in_c, sum_a, sum_b, sum_c, gram_in,
    load_sem, send_sem, recv_sem, gather_sem, send_a, recv_a, send_b, recv_b, send_c, recv_c, gram_send, gram_recv,
):
    me = lax.axis_index("shard")
    feats, samples = data_hbm.shape
    rows = label_ref.shape[2]
    blocks, block = visit_ref.shape
    features = feats * devices
    cubes = devices // 8
    cube = me // 8
    bit0, bit1, bit2 = me % 2, (me // 2) % 2, (me // 4) % 2
    partner = me + 1 - 2 * bit0

    def columns(k):
        return pl.ds(pl.multiple_of(k * rows, rows), rows)

    def loop(first, last, action):
        def step(i, carry):
            action(i)
            return carry

        lax.fori_loop(first, last, step, 0)

    upward = cube // (cubes // 2)

    def near(i):
        place = upward * (cubes - 2 - i) + (1 - upward) * i
        return place + jnp.where(place >= cube, 1, 0)

    def far(i):
        return near(cubes - 2 - i)

    def mates(action):
        loop(1, 8, lambda i: action(8 * cube + lax.rem(me + i, 8)))

    def cube_of(q, action):
        loop(0, 8, lambda j: action(8 * q + j))

    def peers(action):
        loop(0, cubes - 1, lambda i: cube_of(far(i), action))
        mates(action)

    def remote(source, target, send, recv, peer):
        return pltpu.make_async_remote_copy(
            src_ref=source, dst_ref=target, send_sem=send, recv_sem=recv,
            device_id=(peer,), device_id_type=MESH,
        )

    def total_wait(ref, phase):
        view = ref.at[pl.ds(0, devices - 1)]
        return remote(view, view, send_sem.at[phase], recv_sem.at[phase % 3], partner)

    def scatter_send(part, got, phase):
        def send(peer):
            remote(part.at[peer], got.at[me], send_sem.at[phase], recv_sem.at[phase], peer).start()

        return send

    def gather_start(own, everyone, phase):
        everyone[me] = own[...]
        spot = (phase - 3) * cubes + cube
        peers(lambda peer: remote(own, everyone.at[me], send_sem.at[phase], gather_sem.at[spot], peer).start())

    def part_of(lhs, part, q):
        for j in range(8):
            k = 8 * q + j
            part[k, 0:1, :] = nn(lhs, data_ref[:, columns(k)])[0:1, :]

    def margin_scatter(row, part, got, phase):
        lhs = spread(row)
        send = scatter_send(part, got, phase)

        def step(i):
            q = far(i)
            part_of(lhs, part, q)
            cube_of(q, send)

        loop(0, cubes - 1, step)
        part_of(lhs, part, cube)
        mates(send)
        got[me] = part[me]

    def back(everyone, phase):
        def arrival(q, count):
            view = everyone.at[pl.ds(8 * q, count)]
            spot = (phase - 3) * cubes + q
            remote(view, view, send_sem.at[phase], gather_sem.at[spot], partner).wait_recv()

        def cube_sum(q, total):
            for j in range(8):
                k = 8 * q + j
                total = total + nt(spread(everyone[k][0:1, 0:rows]), data_ref[:, columns(k)])
            return total

        def step(i, total):
            q = near(i)
            arrival(q, 8)
            return cube_sum(q, total)

        arrival(cube, 7)
        total = cube_sum(cube, jnp.zeros((ROWS, feats), F32))
        return lax.fori_loop(0, cubes - 1, step, total)[0:1, :]

    def load(q):
        view = pl.ds(pl.multiple_of(8 * q * rows, rows), 8 * rows)
        return pltpu.make_async_copy(data_hbm.at[:, view], data_ref.at[:, view], load_sem.at[q])

    loop(0, cubes - 1, lambda i: load(far(i)).start())
    load(cube).start()
    barrier = pltpu.get_barrier_semaphore()
    peers(lambda peer: pl.semaphore_signal(barrier, inc=1, device_id=(peer,), device_id_type=MESH))

    w_start = start_ref[...]
    sign, bound = label_ref[me].astype(F32), bound_ref[me]
    start_rows = spread(w_start)

    def first_part(q):
        load(q).wait()
        part_of(start_rows, part0, q)

    loop(0, cubes - 1, lambda i: first_part(far(i)))
    first_part(cube)
    pl.semaphore_wait(barrier, devices - 1)
    peers(scatter_send(part0, got0, 0))
    got0[me] = part0[me]

    row_at = lax.broadcasted_iota(jnp.int32, (block, block), 0)
    lane_at = lax.broadcasted_iota(jnp.int32, (block, block), 1)
    upper, lower, even = row_at < lane_at, row_at > lane_at, row_at == lane_at

    def gram_of(k):
        tile = data_ref[:, columns(k)]
        first, second = tile[:, :block], tile[:, block:]
        top = lax.dot_general(first, tile, (((0,), (0,)), ((), ())), preferred_element_type=F32)
        low = lax.dot_general(second, second, (((0,), (0,)), ((), ())), preferred_element_type=F32)
        gram[k, :, :block] = jnp.where(upper, top[:, :block], low).astype(BF16)
        gram[k, :, block:] = top[:, block:].astype(BF16)
        part1[k, 1:2, :block] = jnp.sum(jnp.where(even, top[:, :block], 0.0), axis=0, keepdims=True)
        part1[k, 1:2, block:] = jnp.sum(jnp.where(even, low, 0.0), axis=0, keepdims=True)
        left, right = first.astype(F32), second.astype(F32)
        return left * left + right * right

    def halving(source, target, index, sends, recvs, peer):
        return pltpu.make_async_remote_copy(
            src_ref=source, dst_ref=target.at[index], send_sem=sends.at[index],
            recv_sem=recvs.at[index], device_id=(peer,), device_id_type=MESH,
        )

    def copy_a(q, j):
        return halving(gram.at[8 * q + 2 * j + 1 - bit0], in_a, 4 * q + j, send_a, recv_a, partner)

    def order_of(q):
        swap = q % 2
        return (1 - swap) * bit1 + swap * bit2, 1 + swap, (1 - swap) * bit2 + swap * bit1, 2 - swap

    def copy_b(q, t):
        bit, weight, _, other = order_of(q)
        return halving(
            sum_a.at[4 * q + weight * (1 - bit) + other * t], in_b, 2 * q + t, send_b, recv_b,
            me + 2 * weight * (1 - 2 * bit),
        )

    def copy_c(q):
        _, _, bit, weight = order_of(q)
        return halving(sum_b.at[2 * q + 1 - bit], in_c, q, send_c, recv_c, me + 2 * weight * (1 - 2 * bit))

    def copy_d(q):
        return pltpu.make_async_remote_copy(
            src_ref=sum_c.at[q], dst_ref=gram_in.at[cube], send_sem=gram_send.at[0],
            recv_sem=gram_recv.at[0], device_id=(me + 8 * (q - cube),), device_id_type=MESH,
        )

    def added(x, y):
        return (x.astype(F32) + y.astype(F32)).astype(BF16)

    def turn(i):
        return jnp.where(i == cubes - 1, cube, far(jnp.minimum(i, cubes - 2)))

    def merge_a(i):
        q = turn(i)
        bit, weight, last, other = order_of(q)
        for t in (1 - last, last):
            for side in (1 - bit, bit):
                at = weight * side + other * t
                copy_a(q, at).wait_recv()
                sum_a[4 * q + at] = added(gram[8 * q + 2 * at + bit0], in_a[4 * q + at])
            copy_b(q, t).start()

    def merge_b(i):
        q = turn(i)
        bit, weight, last, other = order_of(q)
        for t in (1 - last, last):
            copy_b(q, t).wait_recv()
            sum_b[2 * q + t] = added(sum_a[4 * q + weight * bit + other * t], in_b[2 * q + t])
        copy_c(q).start()

    def merged_c(q):
        bit = order_of(q)[2]
        copy_c(q).wait_recv()
        return added(sum_b[2 * q + bit], in_c[q])

    def merge_c(i):
        q = turn(i)
        sum_c[q] = merged_c(q)
        copy_d(q).start()

    def gram_step(i, total):
        q = turn(i)
        for j in range(4):
            total = total + gram_of(8 * q + 2 * j + 1 - bit0)
        for j in range(4):
            copy_a(q, j).start()
        for j in range(4):
            total = total + gram_of(8 * q + 2 * j + bit0)
        merge_a(i)
        return total

    half = cubes // 2
    square_total = lax.fori_loop(0, half, gram_step, jnp.zeros((feats, block), F32))
    total_wait(got0, 0).wait_recv()
    margin0 = jnp.sum(got0[...], axis=0)
    own0[...] = bound * sign * jnp.maximum(0.0, 1.0 - sign * margin0)
    gather_start(own0, all0, 0 + 3)

    def late_step(i, total):
        total = gram_step(i, total)
        merge_b(i - half)
        return total

    square_total = lax.fori_loop(half, cubes, late_step, square_total)
    column_sq = nt(jnp.ones((8, block), F32), square_total, HIGH)[0:1, :]
    ascent = back(all0, 3)
    loop(cubes - half, cubes - 1, merge_b)
    scale = column_sq / samples + 1e-06
    stepped = w_start + ascent / (samples * scale)
    thresh = 1.0 / (4.0 * features * scale)
    primal = stepped - jnp.clip(stepped, -thresh, thresh)
    margin_scatter(primal, part1, got1, 1)
    merge_b(cubes - 1)
    loop(0, cubes - 1, merge_c)
    gram_in[cube] = merged_c(cube)

    orders, places = [], []
    for b in range(blocks):
        order = (lax.broadcasted_iota(jnp.int32, (block, block), 0) == visit_ref[b:b + 1, :]).astype(F32)
        orders.append(order)
        places.append(order.T.astype(BF16))

    alpha_zero = bound * frac_ref[...]

    def permute(vectors):
        stacked = jnp.concatenate(list(vectors) + [jnp.zeros((8 - len(vectors), rows), F32)], axis=0)
        return [nn(stacked[:, b * block:(b + 1) * block], orders[b], HIGH) for b in range(blocks)]

    total_wait(got1, 1).wait_recv()
    received = jnp.sum(got1[...], axis=0)
    margin1, diag = received[0:1, :], received[1:2, :]
    loss = jnp.sum(bound * jnp.square(jnp.maximum(0.0, 1.0 - sign * margin1)), axis=1, keepdims=True)
    penalty = jnp.sum(jnp.abs(primal), axis=1, keepdims=True)
    objective_part = loss / (2.0 * samples) + penalty / (4.0 * features)
    permuted = permute((sign, bound, alpha_zero, diag, margin1))
    sign_p = [x[0:1] for x in permuted]
    bound_p = [x[1:2] for x in permuted]
    zero_p = [x[2:3] for x in permuted]
    inverse_p = [0.5 / (x[3:4] + 1e-06) for x in permuted]
    margin_p = [x[4:5] for x in permuted]

    view = gram_in.at[pl.ds(0, cubes - 1)]
    gram_wait = pltpu.make_async_remote_copy(
        src_ref=view, dst_ref=view, send_sem=gram_send.at[0], recv_sem=gram_recv.at[0],
        device_id=(partner,), device_id_type=MESH,
    )
    gram_wait.wait_recv()
    full = jnp.sum(gram_in[...].astype(F32), axis=0)
    packed, cross = full[:, :block], full[:, block:]
    above, below = jnp.where(upper, packed, 0.0), jnp.where(lower, packed, 0.0)
    blocks_p = {}
    for (a, b), piece in {(0, 0): above + above.T, (0, 1): cross, (1, 1): below + below.T}.items():
        piece = nn(piece.astype(BF16), orders[b].astype(BF16)).astype(BF16)
        blocks_p[a, b] = nn(places[a], piece).astype(BF16)

    lane = lax.broadcasted_iota(jnp.int32, (1, block), 1)
    sub = lax.broadcasted_iota(jnp.int32, (ROWS, block), 0)

    def times_gram(delta, piece):
        high = delta.astype(BF16).astype(F32)
        lhs = jnp.where(sub == 0, high, jnp.where(sub == 1, delta - high, 0.0)).astype(BF16)
        return 2.0 * jnp.sum(nn(lhs, piece)[0:8], axis=0, keepdims=True)

    def sweep(alpha, margin):
        result, margin = [], list(margin)
        for b in range(blocks):
            now, m, moved = alpha[b], margin[b], jnp.zeros((1, block), F32)
            for s in range(block // GROUP):
                fresh = jnp.clip(now + (1.0 - sign_p[b] * m) * inverse_p[b], 0.0, bound_p[b])
                mine = (lane >= s * GROUP) & (lane < (s + 1) * GROUP)
                change = jnp.where(mine, fresh - now, 0.0)
                now = jnp.where(mine, fresh, now)
                change = sign_p[b] * change
                moved = moved + change
                if s + 1 < block // GROUP:
                    m = m + times_gram(change, blocks_p[b, b])
            for later in range(b + 1, blocks):
                margin[later] = margin[later] + times_gram(moved, blocks_p[b, later])
            result.append(now)
        return result

    def changes(after, before):
        pieces = []
        for b in range(blocks):
            z = spread(sign_p[b] * (after[b] - before[b]))
            pieces.append(nt(z, orders[b].astype(BF16))[0:1, :])
        return jnp.concatenate(pieces, axis=1)

    one_p = sweep(zero_p, margin_p)
    own1[0:1, 0:rows] = changes(one_p, zero_p)
    own1[0:1, rows:] = jnp.broadcast_to(objective_part, (1, block))
    gather_start(own1, all1, 1 + 3)
    update_one = back(all1, 4) * (2.0 / devices)
    margin_scatter(update_one, part2, got2, 2)
    objective_ref[...] = jnp.sum(all1[...], axis=0)[:, rows:]
    total_wait(got2, 2).wait_recv()
    margin2 = margin1 + jnp.sum(got2[...], axis=0)
    margin2_p = [x[0:1] for x in permute((margin2,))]
    two_p = sweep(one_p, margin2_p)
    own2[...] = changes(two_p, one_p)
    gather_start(own2, all2, 2 + 3)
    for b in range(blocks):
        spot = jnp.broadcast_to(two_p[b], (8, block))
        out_ref[:, feats + b * block:feats + (b + 1) * block] = nt(spot, orders[b], HIGH)[0:1, :]
    out_ref[:, :feats] = primal + update_one + back(all2, 5) * (2.0 / devices)

    for phase, ref in enumerate((got0, got1, got2)):
        total_wait(ref, phase).wait_send()
    for phase, ref in enumerate((all0, all1, all2)):
        total_wait(ref, phase + 3).wait_send()
    gram_wait.wait_send()

    def drain(q):
        for j in range(4):
            copy_a(q, j).wait_send()
        for j in range(2):
            copy_b(q, j).wait_send()
        copy_c(q).wait_send()

    loop(0, cubes, drain)


def body(devices, data_t, labels, sample_weight, w_start, alpha_start, visit_order):
    feats = data_t.shape[0]
    rows = alpha_start.shape[0]
    blocks, block = visit_order.shape
    cubes = devices // 8
    labels = labels.reshape(devices, 1, rows)
    bound = sample_weight.reshape(devices, 1, rows)

    def grams(count):
        return pltpu.VMEM((count, block, rows), BF16)

    def semaphores(count):
        return pltpu.SemaphoreType.DMA((count,))

    def vectors(height, length):
        return pltpu.VMEM((devices, height, length), F32)

    vmem = pl.BlockSpec(memory_space=pltpu.VMEM)
    out, objective = pl.pallas_call(
        functools.partial(kernel, devices),
        name="svm_rounds",
        out_shape=(
            jax.ShapeDtypeStruct((1, feats + rows), F32),
            jax.ShapeDtypeStruct((1, block), F32),
        ),
        in_specs=[pl.BlockSpec(memory_space=pl.ANY)] + [vmem] * 5,
        out_specs=(vmem, vmem),
        scratch_shapes=[
            vectors(1, rows), vectors(2, rows), vectors(1, rows),
            vectors(1, rows), vectors(2, rows), vectors(1, rows),
            pltpu.VMEM((1, rows), F32), pltpu.VMEM((1, rows + block), F32), pltpu.VMEM((1, rows), F32),
            vectors(1, rows), vectors(1, rows + block), vectors(1, rows),
            pltpu.VMEM(data_t.shape, BF16), grams(devices), grams(4 * cubes), grams(2 * cubes), grams(cubes),
            grams(4 * cubes), grams(2 * cubes), grams(cubes), grams(cubes),
            semaphores(cubes), semaphores(6), semaphores(3), semaphores(3 * cubes), semaphores(4 * cubes), semaphores(4 * cubes),
            semaphores(2 * cubes), semaphores(2 * cubes), semaphores(cubes), semaphores(cubes),
            semaphores(1), semaphores(1),
        ],
        compiler_params=pltpu.CompilerParams(
            collective_id=0, has_side_effects=True, vmem_limit_bytes=63 * 1024 * 1024
        ),
    )(data_t, labels, bound, w_start[None], alpha_start[None], visit_order)
    return out[0, :feats], out[0, feats:feats + rows], objective[0, 0]


def solution(mesh):
    placed = (P("shard", None), P(), P(), P("shard"), P("shard"), P("shard", None))
    return jax.shard_map(
        functools.partial(body, mesh.shape["shard"]), mesh=mesh, in_specs=placed,
        out_specs=(P("shard"), P("shard"), P()), check_vma=False,
    )
```
